128 devices in a mesh: seq: 4 (over z_lo, core), mp: 32 (over z_hi, y, x).
Axes of the slice: x: 4, y: 4, z: 4 (z_hi: 2, z_lo: 2; z = z_hi * 2 + z_lo), core: 2. Of those that a mesh axis runs over, the one named last changes fastest.
Arguments:
- byte_states: bfloat16 [4, 16384, 1024], P('seq', 'mp'), may hold values from -312 to 312
- patch_latents: bfloat16 [4, 4096, 4096], P(None, 'seq', 'mp'), may hold values from -6 to 6
- patch_lengths: int32 [4, 4096], P('seq'), may hold values from 1 to 12, 16384 in all within a row
- w_down: bfloat16 [4096, 1024], replicated, may hold values from -0.09375 to 0.09375
- kv_gain: bfloat16 [1024], replicated, may hold values from 0.25 to 1.75
- w_query: bfloat16 [1024, 1024], replicated, may hold values from -0.375 to 0.375
- w_key: bfloat16 [1024, 1024], replicated, may hold values from -0.1875 to 0.1875
- w_value: bfloat16 [1024, 1024], replicated, may hold values from -0.1875 to 0.1875
- w_out: bfloat16 [1024, 1024], replicated, may hold values from -0.375 to 0.375
- out_gain: bfloat16 [1024], replicated, may hold values from 0.25 to 1.75
Outputs:
- decoded: bfloat16 [4, 16384, 1024], P('seq', 'mp')
The draws below stay inside these ranges and needn't reach their ends.
Inputs may be any that keep to these rules, and one draw needn't show every extreme that they name: patch_lengths[s] lists the lengths of the 4096 patches of sequence s in order; they sum to 16384 and the longest is exactly 12.
All inputs are finite; a program needn't handle non-finite values.
Results may differ from the reference program's by a relative error of at most 0.0076.
Values may be sent and summed in bfloat16 or wider, within the bound.
No kernel may reach another device: no remote copies, remote signals or barrier semaphores. Data moves between devices by JAX's collectives and lax.ppermute only.
A program may use at most 128 MiB of HBM per device.

```python
import math
import jax
import jax.numpy as jnp
import numpy as np
from jax import lax

D = 1024
GD = 4096
HEADS = 16
HEAD_DIM = 64
MOST = 12
SEQ_LEN = 16384
PATCHES = 4096
SEQS = 4


def draw_byte_states(key, part):
    base_key = jax.random.fold_in(key, 0)
    values = jnp.clip(jax.random.normal(base_key, (SEQS, SEQ_LEN, D), jnp.float32), -6.0, 6.0)
    return values.astype(jnp.bfloat16)


def steps_of(own_key, dims, cuts, least, largest):
    level, own = 1.0, jax.random.fold_in(own_key, 6)
    for dim, parts in cuts:
        heights = jnp.exp(jax.random.uniform(jax.random.fold_in(own, dim), (parts,), jnp.float32, least / len(cuts), largest / len(cuts)))
        level = level * jnp.repeat(heights, dims[dim] // parts).reshape([-1 if axis == dim else 1 for axis in range(len(dims))])
    return level


def length_profile(amount, total, reach, skew):
    loads = [(1 << 20) // math.isqrt(standing ** skew) + 1 for standing in range(2, amount + 1)]
    rest, holding = total - reach - (amount - 1), [1] * (amount - 1)
    while rest > 0:
        free = [i for i in range(amount - 1) if holding[i] < reach]
        pool, left = sum([loads[i] for i in free]), rest
        for i in free:
            extra = min(reach - holding[i], max(1, left * loads[i] // pool), rest)
            holding[i] = holding[i] + extra
            rest = rest - extra
    return np.array([reach] + holding)


def ragged_sizes(stream_key, amount, total, bound, skew):
    if amount == 2:
        one = jax.random.randint(stream_key, (), max(1, total - bound), min(bound, total - 1) + 1)
        return jnp.stack([one, total - one])
    sizes = jnp.asarray(length_profile(amount, total, bound, skew), jnp.int32)
    twos = (amount - 1) // 2
    donor, taker = sizes[1:1 + 2 * twos:2], sizes[2:2 + 2 * twos:2]
    room = jnp.minimum(donor - 1, bound - taker)
    passed = jax.random.randint(jax.random.fold_in(stream_key, 1), (twos,), 0, 1 << 20) % (room + 1)
    sizes = sizes.at[1:1 + 2 * twos:2].set(donor - passed).at[2:2 + 2 * twos:2].set(taker + passed)
    return sizes[jax.random.permutation(jax.random.fold_in(stream_key, 2), amount)]


def centred(rng, shape, width, reach, shards=(), kind=jnp.bfloat16):
    entries = width * jax.random.normal(rng, shape, jnp.float32)
    if shards:
        entries = entries * steps_of(rng, shape, shards, -0.22, 0.18)
    return jnp.clip(entries, -reach, reach).astype(kind)


def setup_inputs(seed: int = 0) -> dict:
    seeds = jax.random.split(jax.random.key(seed), 11)
    return {
        "byte_states": draw_byte_states(jax.random.fold_in(seeds[10], 71), 0),
        "patch_latents": centred(seeds[1], (SEQS, PATCHES, GD), 1.0, 6.0, ((1, 4), (2, 32))),
        "patch_lengths": jax.vmap(lambda own: ragged_sizes(own, PATCHES, SEQ_LEN, MOST, 2))(jax.random.split(seeds[2], SEQS)).reshape((SEQS, PATCHES)).astype(jnp.int32),
        "w_down": centred(seeds[3], (GD, D), GD ** -0.5, 0.09375),
        "kv_gain": jnp.clip(1.0 + 0.15 * jax.random.normal(seeds[4], (D,), jnp.float32), 0.25, 1.75).astype(jnp.bfloat16),
        "w_query": centred(seeds[5], (D, D), (D // 4) ** -0.5, 0.375),
        "w_key": centred(seeds[6], (D, D), D ** -0.5, 0.1875),
        "w_value": centred(seeds[7], (D, D), D ** -0.5, 0.1875),
        "w_out": centred(seeds[8], (D, D), (D // 4) ** -0.5, 0.375),
        "out_gain": jnp.clip(1.0 + 0.15 * jax.random.normal(seeds[9], (D,), jnp.float32), 0.25, 1.75).astype(jnp.bfloat16),
    }


def rms_norm(values, gain_row):
    mean_square = lax.optimization_barrier(jnp.mean(values * values, axis=-1, keepdims=True))
    return values * lax.rsqrt(mean_square + 1e-05) * gain_row.astype(jnp.float32)

def attend(query_block, position_block, key_rows, value_rows, starts):
    row_count = query_block.shape[0]
    scale_factor = 1.0 / math.sqrt(HEAD_DIM)
    query_heads = query_block.astype(jnp.float32).reshape(row_count, HEADS, HEAD_DIM)
    key_heads = key_rows.astype(jnp.float32).reshape(-1, HEADS, HEAD_DIM)
    value_heads = value_rows.astype(jnp.float32).reshape(-1, HEADS, HEAD_DIM)
    scores = jnp.einsum('rhd,khd->hrk', query_heads, key_heads) * scale_factor
    allowed = starts[None, None, :] <= position_block[None, :, None]
    masked = jnp.where(allowed, scores, -1e+30)
    row_max = lax.optimization_barrier(jnp.max(masked, axis=-1, keepdims=True))
    raised = jnp.where(allowed, jnp.exp(masked - row_max), 0.0)
    totals = lax.optimization_barrier(jnp.sum(raised, axis=-1))
    weights = raised.astype(jnp.bfloat16).astype(jnp.float32)
    summed = jnp.einsum('hrk,khd->hrd', weights, value_heads) / totals[..., None]
    return jnp.transpose(summed, (1, 0, 2)).reshape(row_count, D).astype(jnp.bfloat16)

def reference(byte_states, patch_latents, patch_lengths, w_down, kv_gain, w_query, w_key, w_value, w_out, out_gain):
    decoded_rows = []
    block_rows = math.gcd(SEQ_LEN, 512)
    for sequence in range(SEQS):
        projected = jnp.dot(patch_latents[sequence], w_down, preferred_element_type=jnp.float32)
        patch_normed = rms_norm(projected, kv_gain).astype(jnp.bfloat16)
        key_rows = jnp.dot(patch_normed, w_key, preferred_element_type=jnp.float32).astype(jnp.bfloat16)
        value_rows = jnp.dot(patch_normed, w_value, preferred_element_type=jnp.float32).astype(jnp.bfloat16)
        lengths = patch_lengths[sequence].astype(jnp.int32)
        starts = jnp.cumsum(lengths).astype(jnp.int32) - lengths
        queries = jnp.dot(byte_states[sequence], w_query, preferred_element_type=jnp.float32).astype(jnp.bfloat16)
        query_blocks = queries.reshape(SEQ_LEN // block_rows, block_rows, D)
        position_blocks = jnp.arange(SEQ_LEN, dtype=jnp.int32).reshape(SEQ_LEN // block_rows, block_rows)

        def attend_rows(packed):
            return attend(packed[0], packed[1], key_rows, value_rows, starts)
        head_out = lax.map(attend_rows, (query_blocks, position_blocks)).reshape(SEQ_LEN, D)
        residual = byte_states[sequence].astype(jnp.float32) + jnp.dot(head_out, w_out, preferred_element_type=jnp.float32)
        decoded_rows.append(rms_norm(residual, out_gain).astype(jnp.bfloat16))
    return jnp.stack(decoded_rows)
```

```python
import functools
import math

import jax
import jax.numpy as jnp
from jax import lax
from jax.experimental import pallas as pl
from jax.experimental.pallas import tpu as pltpu
from jax.sharding import PartitionSpec as P

HEADS = 16
HEAD_DIM = 64
BLOCK_ROWS = 256
KEY_TILE = 512
UNROLL = 4
SUM_ROWS = 16
TO_LOG2 = math.log2(math.e) / math.sqrt(HEAD_DIM)
SCALE = 1.0 / math.sqrt(HEAD_DIM)
LEAST_TOTAL = 2.0**-90
MOST_TOTAL = 2.0**110
MIB = 1024 * 1024


def vmem():
    return pl.BlockSpec(memory_space=pltpu.VMEM)


def smem():
    return pl.BlockSpec(memory_space=pltpu.SMEM)


def query_kernel(x_ref, w_ref, len_ref, q_ref, starts_ref):
    rows, width = x_ref.shape
    lengths = len_ref[...].astype(jnp.float32).astype(jnp.bfloat16)
    lines, lanes = lengths.shape
    before = (
        lax.broadcasted_iota(jnp.int32, (lanes, lanes), 0)
        < lax.broadcasted_iota(jnp.int32, (lanes, lanes), 1)
    )
    within = jnp.dot(
        lengths, before.astype(jnp.float32).astype(jnp.bfloat16), preferred_element_type=jnp.float32
    )
    above = (
        lax.broadcasted_iota(jnp.int32, (lines, lines), 1)
        < lax.broadcasted_iota(jnp.int32, (lines, lines), 0)
    )
    column_sums = jnp.dot(
        above.astype(jnp.float32).astype(jnp.bfloat16), lengths, preferred_element_type=jnp.float32
    )
    starts_ref[...] = (within + jnp.sum(column_sums, axis=1, keepdims=True)).astype(jnp.int32)
    step = 256
    heads_step = step // HEAD_DIM
    for n in range(width // step):
        q = jnp.dot(
            x_ref[...], w_ref[:, n * step : (n + 1) * step], preferred_element_type=jnp.float32
        ).astype(jnp.bfloat16)
        qt = q.T
        for r in range(rows // BLOCK_ROWS):
            part = qt[:, r * BLOCK_ROWS : (r + 1) * BLOCK_ROWS]
            q_ref[r, n * heads_step : (n + 1) * heads_step] = part.reshape(
                heads_step, HEAD_DIM, BLOCK_ROWS
            )


def query_call(x, w_query, lengths):
    rows, width = x.shape
    copies = rows // BLOCK_ROWS
    return pl.pallas_call(
        query_kernel,
        out_shape=(
            jax.ShapeDtypeStruct((copies, HEADS, HEAD_DIM, BLOCK_ROWS), jnp.bfloat16),
            jax.ShapeDtypeStruct(lengths.shape, jnp.int32),
        ),
        in_specs=[vmem(), vmem(), vmem()],
        out_specs=(vmem(), vmem()),
        compiler_params=pltpu.CompilerParams(vmem_limit_bytes=16 * MIB),
        cost_estimate=pl.CostEstimate(
            flops=2 * rows * width * width, bytes_accessed=2 * (2 * rows * width + width * width),
            transcendentals=0,
        ),
        name="queries",
    )(x, w_query, lengths)


def norm_rows(values, gain):
    mean_square = jnp.mean(values * values, axis=-1, keepdims=True)
    return values * lax.rsqrt(mean_square + 1e-05) * gain.astype(jnp.float32)


def kv_kernel(x_ref, wd_ref, gain_ref, wk_ref, wv_ref, out_ref):
    blocks, groups, part, lanes = x_ref.shape
    rows = blocks * part
    width = wd_ref.shape[1]
    lhs = jnp.concatenate([x_ref[:, g].reshape(rows, lanes) for g in range(groups)], axis=1)
    projected = jnp.dot(lhs, wd_ref[...], preferred_element_type=jnp.float32)
    normed = norm_rows(projected, gain_ref[...]).astype(jnp.bfloat16)
    keys = jnp.dot(normed, wk_ref[...], preferred_element_type=jnp.float32)
    values = jnp.dot(normed, wv_ref[...], preferred_element_type=jnp.float32)
    copies = out_ref.shape[0]
    for h in range(width // HEAD_DIM):
        cut = slice(h * HEAD_DIM, (h + 1) * HEAD_DIM)
        both = jnp.concatenate([keys[:, cut], values[:, cut]], axis=1).astype(jnp.bfloat16)
        for r in range(copies):
            out_ref[r, h] = both


def kv_call(x, w_down, gain, w_key, w_value, copies):
    blocks, groups, part, lanes = x.shape
    rows = blocks * part
    width = w_down.shape[1]
    return pl.pallas_call(
        kv_kernel,
        out_shape=jax.ShapeDtypeStruct((copies, HEADS, rows, 2 * HEAD_DIM), jnp.bfloat16),
        in_specs=[vmem()] * 5,
        out_specs=vmem(),
        compiler_params=pltpu.CompilerParams(vmem_limit_bytes=32 * MIB),
        cost_estimate=pl.CostEstimate(
            flops=2 * rows * width * (groups * lanes + 2 * width),
            bytes_accessed=2 * (rows * groups * lanes + groups * lanes * width + 2 * width * width),
            transcendentals=0,
        ),
        name="keys_values",
    )(x, w_down, gain.reshape(1, -1), w_key, w_value)


def attend_kernel(
    group_ref, starts_s_ref, starts_ref, kv_ref, q_ref, out_ref,
    kvs, vt, qa, starts_b, acc, probs, flag,
):
    senders, blocks, part, lanes = kv_ref.shape
    row_blocks = q_ref.shape[0]
    patches = senders * blocks * part
    key_tiles = patches // KEY_TILE
    stride = q_ref.shape[2] * group_ref[1]
    group = group_ref[0]

    def first_row(m):
        return m * stride + group * BLOCK_ROWS

    for b in range(blocks):
        for s in range(senders):
            at = (b * senders + s) * part
            kvs[at : at + part, :] = kv_ref[s, b]
    for t in range(key_tiles):
        turned = kvs[t * KEY_TILE : (t + 1) * KEY_TILE, :].T
        vt[t, :HEAD_DIM, :] = turned[HEAD_DIM:, :]
        vt[t, HEAD_DIM:, :] = jnp.ones((SUM_ROWS, KEY_TILE), jnp.bfloat16)
    for line in range(patches // 128):
        row = jnp.broadcast_to(starts_ref[line : line + 1, :], (128, 128))
        starts_b[line * 128 : (line + 1) * 128, :] = row.T
    zeros = jnp.zeros((HEAD_DIM, BLOCK_ROWS), jnp.bfloat16)

    def prepare(m, carry):
        qa[m, :HEAD_DIM, :] = q_ref[m]
        qa[m, HEAD_DIM:, :] = zeros
        acc[m] = jnp.zeros(acc.shape[1:], jnp.float32)
        return carry

    lax.fori_loop(0, row_blocks, prepare, 0)
    qa[row_blocks] = jnp.zeros(qa.shape[1:], jnp.bfloat16)
    acc[row_blocks] = jnp.zeros(acc.shape[1:], jnp.float32)

    def ceil_blocks(rows):
        return jnp.minimum((jnp.maximum(rows, 0) + stride - 1) // stride, row_blocks)

    def lowest(kt):
        at = kt * KEY_TILE
        start = starts_s_ref[at // 128, 0]
        return ceil_blocks(start - group * BLOCK_ROWS - (BLOCK_ROWS - 1))

    def lowest_full(kt):
        at = kt * KEY_TILE + KEY_TILE - 1
        start = starts_s_ref[at // 128, 127]
        return ceil_blocks(start - group * BLOCK_ROWS)

    def weigh(kt, m, masked):
        keys = kvs[pl.ds(pl.multiple_of(kt * KEY_TILE, KEY_TILE), KEY_TILE), :]
        scores = jnp.dot(keys, qa[m], preferred_element_type=jnp.float32)
        p = jnp.exp2(scores * TO_LOG2)
        if masked:
            first = starts_b[pl.ds(pl.multiple_of(kt * KEY_TILE, KEY_TILE), KEY_TILE), :]
            first = jnp.concatenate([first] * (BLOCK_ROWS // 128), axis=1)
            rows = first_row(m) + lax.broadcasted_iota(jnp.int32, (KEY_TILE, BLOCK_ROWS), 1)
            p = jnp.where(first <= rows, p, 0.0)
        return p.astype(jnp.bfloat16)

    def fold(kt, m, p):
        acc[m] = acc[m] + jnp.dot(vt[kt], p, preferred_element_type=jnp.float32)

    def run(masked, first_of, past_of):
        total = jnp.int32(0)
        for kt in range(key_tiles):
            total = total + jnp.maximum(past_of(kt) - first_of(kt), 0)

        def settle(kt, m):
            def more(state):
                kt, m = state
                return jnp.logical_and(kt < key_tiles, m >= past_of(jnp.minimum(kt, key_tiles - 1)))

            def on(state):
                kt, _ = state
                return kt + 1, first_of(jnp.minimum(kt + 1, key_tiles - 1))

            return lax.while_loop(more, on, (kt, m))

        def advance(kt, m):
            return settle(kt, m + 1)

        def usable(kt, m):
            valid = kt < key_tiles
            return jnp.where(valid, kt, 0), jnp.where(valid, m, row_blocks)

        steps = (total + UNROLL - 1) // UNROLL
        start = settle(jnp.int32(0), first_of(0))

        def take(state):
            pairs = []
            for _ in range(UNROLL):
                pairs.append(usable(*state))
                state = advance(*state)
            return pairs, state

        @pl.when(total > 0)
        def _():
            pairs, state = take(start)
            for i, (kt, m) in enumerate(pairs):
                probs[i] = weigh(kt, m, masked)

            def body(_, carry):
                state, flat = carry
                old = [(flat[2 * i], flat[2 * i + 1]) for i in range(UNROLL)]
                pairs, state = take(state)
                for i in range(UNROLL):
                    ready = probs[i]
                    fold(*old[i], ready)
                    probs[i] = weigh(*pairs[i], masked)
                return state, tuple(v for pair in pairs for v in pair)

            flat = tuple(v for pair in pairs for v in pair)
            _, flat = lax.fori_loop(0, steps - 1, body, (state, flat))
            for i in range(UNROLL):
                fold(flat[2 * i], flat[2 * i + 1], probs[i])

    run(False, lowest_full, lambda kt: jnp.int32(row_blocks))
    run(True, lowest, lowest_full)

    def finish(m, worst):
        totals = acc[m, HEAD_DIM : HEAD_DIM + 1, :]
        out_ref[m] = (acc[m, :HEAD_DIM, :] * (1.0 / totals)).astype(jnp.bfloat16)
        fine = jnp.logical_and(totals > LEAST_TOTAL, totals < MOST_TOTAL)
        return jnp.maximum(worst, jnp.where(fine, 0.0, 1.0))

    worst = lax.fori_loop(0, row_blocks, finish, jnp.zeros((1, BLOCK_ROWS), jnp.float32))
    flag[0] = jnp.max(worst)

    @pl.when(flag[0] > 0.0)
    def _():
        def redo(m, carry):
            rows = first_row(m) + lax.broadcasted_iota(jnp.int32, (KEY_TILE, BLOCK_ROWS), 1)

            def masked_scores(kt):
                at = pl.ds(pl.multiple_of(kt * KEY_TILE, KEY_TILE), KEY_TILE)
                scores = jnp.dot(kvs[at, :], qa[m], preferred_element_type=jnp.float32) * SCALE
                first = jnp.concatenate([starts_b[at, :]] * (BLOCK_ROWS // 128), axis=1)
                return scores, first <= rows

            def fold_max(kt, peak):
                scores, allowed = masked_scores(kt)
                masked = jnp.where(allowed, scores, -3e38)
                return jnp.maximum(peak, jnp.max(masked, axis=0, keepdims=True))

            peak = lax.fori_loop(
                0, key_tiles, fold_max, jnp.full((1, BLOCK_ROWS), -3e38, jnp.float32)
            )
            acc[m] = jnp.zeros(acc.shape[1:], jnp.float32)

            def fold_sum(kt, inner):
                scores, allowed = masked_scores(kt)
                p = jnp.where(allowed, jnp.exp(jnp.where(allowed, scores - peak, 0.0)), 0.0)
                fold(kt, m, p.astype(jnp.bfloat16))
                return inner

            lax.fori_loop(0, key_tiles, fold_sum, 0)
            totals = acc[m, HEAD_DIM : HEAD_DIM + 1, :]
            out_ref[m] = (acc[m, :HEAD_DIM, :] * (1.0 / totals)).astype(jnp.bfloat16)
            return carry

        lax.fori_loop(0, row_blocks, redo, 0)


def attend_call(group, starts, kv, q):
    senders, blocks, part, lanes = kv.shape
    row_blocks = q.shape[0]
    patches = senders * blocks * part
    key_tiles = patches // KEY_TILE
    return pl.pallas_call(
        attend_kernel,
        out_shape=jax.ShapeDtypeStruct(q.shape, jnp.bfloat16),
        in_specs=[smem(), smem(), vmem(), vmem(), vmem()],
        out_specs=vmem(),
        scratch_shapes=[
            pltpu.VMEM((patches, lanes), jnp.bfloat16),
            pltpu.VMEM((key_tiles, HEAD_DIM + SUM_ROWS, KEY_TILE), jnp.bfloat16),
            pltpu.VMEM((row_blocks + 1, 2 * HEAD_DIM, BLOCK_ROWS), jnp.bfloat16),
            pltpu.VMEM((patches, 128), jnp.int32),
            pltpu.VMEM((row_blocks + 1, HEAD_DIM + SUM_ROWS, BLOCK_ROWS), jnp.float32),
            pltpu.VMEM((UNROLL, KEY_TILE, BLOCK_ROWS), jnp.bfloat16),
            pltpu.SMEM((1,), jnp.float32),
        ],
        compiler_params=pltpu.CompilerParams(vmem_limit_bytes=32 * MIB),
        cost_estimate=pl.CostEstimate(
            flops=2 * patches * row_blocks * BLOCK_ROWS * 2 * HEAD_DIM,
            bytes_accessed=2 * (kv.size + 2 * q.size),
            transcendentals=patches * row_blocks * BLOCK_ROWS // 2,
        ),
        name="attend",
    )(group, starts, starts, kv, q)


def out_kernel(h_ref, w_ref, x_ref, gain_ref, out_ref):
    copies = h_ref.shape[0]
    width = w_ref.shape[0]
    for r in range(copies):
        cut = slice(r * BLOCK_ROWS, (r + 1) * BLOCK_ROWS)
        head_out = h_ref[r].reshape(width, BLOCK_ROWS).T
        residual = x_ref[cut, :].astype(jnp.float32) + jnp.dot(
            head_out, w_ref[...], preferred_element_type=jnp.float32
        )
        out_ref[cut, :] = norm_rows(residual, gain_ref[...]).astype(jnp.bfloat16)


def out_call(head_out, w_out, x, gain):
    rows, width = x.shape
    return pl.pallas_call(
        out_kernel,
        out_shape=jax.ShapeDtypeStruct(x.shape, jnp.bfloat16),
        in_specs=[vmem()] * 4,
        out_specs=vmem(),
        compiler_params=pltpu.CompilerParams(vmem_limit_bytes=16 * MIB),
        cost_estimate=pl.CostEstimate(
            flops=2 * rows * width * width, bytes_accessed=2 * (3 * rows * width + width * width),
            transcendentals=rows,
        ),
        name="outputs",
    )(head_out, w_out, x, gain.reshape(1, -1))


def per_device(
    byte_states, patch_latents, patch_lengths, w_down, kv_gain, w_query, w_key, w_value, w_out,
    out_gain,
):
    seqs, mps = lax.axis_size("seq"), lax.axis_size("mp")
    copies = mps // HEADS
    x = byte_states[0]
    patches_here, features = patch_latents.shape[1:]
    part = patches_here // mps

    sent = patch_latents.reshape(seqs * mps, part, features)
    latents = lax.all_to_all(sent, ("seq", "mp"), 0, 0, tiled=True)
    latents = latents.reshape(seqs, mps, part, features)
    lengths = patch_lengths[0].reshape(-1, 128)
    queries, starts = query_call(x, w_query, lengths)
    queries = queries.reshape(mps, HEAD_DIM, BLOCK_ROWS)
    queries = lax.all_to_all(queries, "mp", 0, 0, tiled=True)

    kv = kv_call(latents, w_down, kv_gain, w_key, w_value, copies)
    kv = lax.all_to_all(kv.reshape(mps, seqs * part, 2 * HEAD_DIM), "mp", 0, 0, tiled=True)
    kv = kv.reshape(mps, seqs, part, 2 * HEAD_DIM)

    group = jnp.stack([lax.axis_index("mp") // HEADS, jnp.int32(copies)])
    head_out = attend_call(group, starts, kv, queries)
    head_out = lax.all_to_all(head_out, "mp", 0, 0, tiled=True)
    decoded = out_call(
        head_out.reshape(copies, HEADS, HEAD_DIM, BLOCK_ROWS), w_out, x, out_gain
    )
    return decoded[None]


def solution(mesh):
    return jax.shard_map(
        per_device,
        mesh=mesh,
        in_specs=(
            P("seq", "mp", None),
            P(None, "seq", "mp"),
            P("seq", None),
            P(),
            P(),
            P(),
            P(),
            P(),
            P(),
            P(),
        ),
        out_specs=P("seq", "mp", None),
        check_vma=False,
    )
```

```python
import functools
import math

import jax
import jax.numpy as jnp
from jax import lax
from jax.experimental import pallas as pl
from jax.experimental.pallas import tpu as pltpu
from jax.sharding import PartitionSpec as P

HEADS = 16
HEAD_DIM = 64
BLOCK_ROWS = 256
KEY_TILE = 512
UNROLL = 8
SUM_ROWS = 16
TO_LOG2 = math.log2(math.e) / math.sqrt(HEAD_DIM)
SCALE = 1.0 / math.sqrt(HEAD_DIM)
LEAST_TOTAL = 2.0**-90
MOST_TOTAL = 2.0**110
MIB = 1024 * 1024


def vmem():
    return pl.BlockSpec(memory_space=pltpu.VMEM)


def smem():
    return pl.BlockSpec(memory_space=pltpu.SMEM)


def hbm():
    return pl.BlockSpec(memory_space=pltpu.HBM)


def ones_where(mask):
    return mask.astype(jnp.float32).astype(jnp.bfloat16)


def iota(shape, dim):
    return lax.broadcasted_iota(jnp.int32, shape, dim)


def exact_dot(a, b):
    return jnp.dot(a, b, preferred_element_type=jnp.float32)


def patch_tables(lengths, starts_ref, counts_ref):
    lines, lanes = lengths.shape
    values = lengths.astype(jnp.float32).astype(jnp.bfloat16)
    square = (lanes, lanes)
    within = exact_dot(values, ones_where(iota(square, 0) < iota(square, 1)))
    small = (lines, lines)
    above = exact_dot(ones_where(iota(small, 1) < iota(small, 0)), values)
    starts = (within + jnp.sum(above, axis=1, keepdims=True)).astype(jnp.int32)
    starts_ref[...] = starts
    spots = counts_ref.shape[0]
    tops, lows = [], []
    for line in range(lines):
        row = starts[line : line + 1, :]
        tops.append(ones_where(iota((spots, lanes), 0) == lax.shift_right_logical(row, 7)))
        lows.append(ones_where(iota((128, lanes), 0) == jnp.bitwise_and(row, 127)))
    present = lax.dot_general(
        jnp.concatenate(tops, axis=1),
        jnp.concatenate(lows, axis=1),
        (((1,), (1,)), ((), ())),
        preferred_element_type=jnp.float32,
    ).astype(jnp.bfloat16)
    along = exact_dot(present, ones_where(iota((128, 128), 0) <= iota((128, 128), 1)))
    before = exact_dot(ones_where(iota((spots, spots), 1) < iota((spots, spots), 0)), present)
    counts_ref[...] = (along + jnp.sum(before, axis=1, keepdims=True)).astype(jnp.int32)


def query_kernel(x_ref, w_ref, len_ref, buf_ref, starts_ref, counts_ref, staged, sems):
    rows, width = x_ref.shape
    step = 256
    heads_step = step // HEAD_DIM
    copies = rows // BLOCK_ROWS
    half = BLOCK_ROWS // 128
    sent = []
    for n in range(width // step):
        q = jnp.dot(
            x_ref[...], w_ref[:, n * step : (n + 1) * step], preferred_element_type=jnp.float32
        ).astype(jnp.bfloat16)
        qt = q.T
        for r in range(copies):
            for h in range(heads_step):
                for b in range(half):
                    at = r * BLOCK_ROWS + b * 128
                    staged[r, n * heads_step + h, b * HEAD_DIM : (b + 1) * HEAD_DIM, :] = qt[
                        h * HEAD_DIM : (h + 1) * HEAD_DIM, at : at + 128
                    ]
            cut = pl.ds(n * heads_step, heads_step)
            send = pltpu.make_async_copy(
                staged.at[r, cut],
                buf_ref.at[pl.ds(r * HEADS + n * heads_step, heads_step), pl.ds(128, 128)],
                sems.at[n * copies + r],
            )
            send.start()
            sent.append(send)
    patch_tables(len_ref[...], starts_ref, counts_ref)
    for send in sent:
        send.wait()


def query_call(x, w_query, lengths, seq_len):
    rows, width = x.shape
    copies = rows // BLOCK_ROWS
    return pl.pallas_call(
        query_kernel,
        out_shape=(
            jax.ShapeDtypeStruct((copies * HEADS, 256, 128), jnp.bfloat16),
            jax.ShapeDtypeStruct(lengths.shape, jnp.int32),
            jax.ShapeDtypeStruct((seq_len // 128, 128), jnp.int32),
        ),
        in_specs=[vmem(), vmem(), vmem()],
        out_specs=(hbm(), vmem(), vmem()),
        scratch_shapes=[
            pltpu.VMEM((copies, HEADS, 128, 128), jnp.bfloat16),
            pltpu.SemaphoreType.DMA((copies * width // 256,)),
        ],
        compiler_params=pltpu.CompilerParams(vmem_limit_bytes=16 * MIB),
        cost_estimate=pl.CostEstimate(
            flops=2 * rows * width * width, bytes_accessed=2 * (2 * rows * width + width * width),
            transcendentals=0,
        ),
        name="queries",
    )(x, w_query, lengths)


def norm_rows(values, gain):
    mean_square = jnp.mean(values * values, axis=-1, keepdims=True)
    return values * lax.rsqrt(mean_square + 1e-05) * gain.astype(jnp.float32)


WD_PARTS = 8


def kv_kernel(
    x_ref, wd_ref, gain_ref, wk_ref, wv_ref, old_ref, buf_ref, wd, wk, wv, acc, staged, sems, outs
):
    blocks, groups, part, lanes = x_ref.shape
    rows = blocks * part
    depth = wd_ref.shape[0] // WD_PARTS
    per_part = groups // WD_PARTS
    loads = [
        pltpu.make_async_copy(
            wd_ref.at[pl.ds(i * depth, depth)], wd.at[pl.ds(i * depth, depth)], sems.at[i]
        )
        for i in range(WD_PARTS)
    ]
    loads.append(pltpu.make_async_copy(wk_ref, wk, sems.at[WD_PARTS]))
    loads.append(pltpu.make_async_copy(wv_ref, wv, sems.at[WD_PARTS + 1]))
    for load in loads:
        load.start()
    for i in range(WD_PARTS):
        lhs = jnp.concatenate(
            [x_ref[:, i * per_part + g].reshape(rows, lanes) for g in range(per_part)], axis=1
        )
        loads[i].wait()
        product = jnp.dot(
            lhs, wd[i * depth : (i + 1) * depth, :], preferred_element_type=jnp.float32
        )
        acc[...] = product if i == 0 else acc[...] + product
    normed = norm_rows(acc[...], gain_ref[...]).astype(jnp.bfloat16)
    loads[WD_PARTS].wait()
    loads[WD_PARTS + 1].wait()
    copies = buf_ref.shape[0] // HEADS
    step = 256
    heads_step = step // HEAD_DIM
    sent = []
    for n in range(wk.shape[1] // step):
        cut = slice(n * step, (n + 1) * step)
        keys = jnp.dot(normed, wk[:, cut], preferred_element_type=jnp.float32)
        values = jnp.dot(normed, wv[:, cut], preferred_element_type=jnp.float32)
        for h in range(heads_step):
            own = slice(h * HEAD_DIM, (h + 1) * HEAD_DIM)
            staged[n * heads_step + h] = jnp.concatenate(
                [keys[:, own], values[:, own]], axis=1
            ).astype(jnp.bfloat16)
        for r in range(copies):
            send = pltpu.make_async_copy(
                staged.at[pl.ds(n * heads_step, heads_step)],
                buf_ref.at[pl.ds(r * HEADS + n * heads_step, heads_step), pl.ds(0, 128)],
                outs.at[n * copies + r],
            )
            send.start()
            sent.append(send)
    for send in sent:
        send.wait()


def kv_call(x, w_down, gain, w_key, w_value, buf):
    blocks, groups, part, lanes = x.shape
    rows = blocks * part
    width = w_down.shape[1]
    return pl.pallas_call(
        kv_kernel,
        out_shape=jax.ShapeDtypeStruct(buf.shape, buf.dtype),
        in_specs=[vmem(), hbm(), vmem(), hbm(), hbm(), hbm()],
        out_specs=hbm(),
        input_output_aliases={5: 0},
        scratch_shapes=[
            pltpu.VMEM(w_down.shape, jnp.bfloat16),
            pltpu.VMEM(w_key.shape, jnp.bfloat16),
            pltpu.VMEM(w_value.shape, jnp.bfloat16),
            pltpu.VMEM((rows, width), jnp.float32),
            pltpu.VMEM((HEADS, rows, 2 * HEAD_DIM), jnp.bfloat16),
            pltpu.SemaphoreType.DMA((WD_PARTS + 2,)),
            pltpu.SemaphoreType.DMA((buf.shape[0] // HEADS * width // 256,)),
        ],
        compiler_params=pltpu.CompilerParams(vmem_limit_bytes=50 * MIB),
        cost_estimate=pl.CostEstimate(
            flops=2 * rows * width * (groups * lanes + 2 * width),
            bytes_accessed=2 * (rows * groups * lanes + groups * lanes * width + 2 * width * width),
            transcendentals=0,
        ),
        name="keys_values",
    )(x, w_down, gain.reshape(1, -1), w_key, w_value, buf)


def attend_kernel(
    blocks, group_ref, starts_ref, counts_ref, in_ref, out_ref,
    kvs, vt, order, acc, probs, staged, lows, flag, sems,
):
    row_blocks = in_ref.shape[0]
    senders = row_blocks
    part = 128 // blocks
    patches = kvs.shape[0]
    key_tiles = patches // KEY_TILE
    stride = BLOCK_ROWS * group_ref[1]
    group = group_ref[0]

    def ceil_blocks(rows):
        return jnp.minimum((jnp.maximum(rows, 0) + stride - 1) // stride, row_blocks)

    total = jnp.int32(0)
    for kt in range(lows.shape[0]):
        if kt < key_tiles:
            start = starts_ref[kt * KEY_TILE // 128, 0]
            low = ceil_blocks(start - group * BLOCK_ROWS - (BLOCK_ROWS - 1))
            total = total + row_blocks - low
        else:
            low = jnp.int32(row_blocks)
        lows[kt] = low

    for b in range(blocks):
        for s in range(senders):
            at = (b * senders + s) * part
            kvs[at : at + part, :] = in_ref[s, b * part : (b + 1) * part, :]
    for t in range(key_tiles):
        turned = kvs[t * KEY_TILE : (t + 1) * KEY_TILE, :].T
        vt[t, :HEAD_DIM, :] = turned[HEAD_DIM:, :]
        vt[t, HEAD_DIM:, :] = jnp.ones((SUM_ROWS, KEY_TILE), jnp.bfloat16)
    order[...] = iota(order.shape, 0)

    def clear(m, carry):
        acc[m] = jnp.zeros(acc.shape[1:], jnp.float32)
        return carry

    lax.fori_loop(0, row_blocks + 1, clear, 0)
    zeros = jnp.zeros((HEAD_DIM, BLOCK_ROWS), jnp.bfloat16)
    lanes = BLOCK_ROWS // 128

    def query_rows(m):
        halves = [
            in_ref[m, 128 + b * HEAD_DIM : 128 + (b + 1) * HEAD_DIM, :] for b in range(lanes)
        ]
        return jnp.concatenate([jnp.concatenate(halves, axis=1), zeros], axis=0)

    def allowed_keys(m, kt):
        line = (m * stride + group * BLOCK_ROWS) // 128
        met = [counts_ref[pl.ds(line + b, 1), :] for b in range(lanes)]
        here = jnp.concatenate(met, axis=1) - kt * KEY_TILE
        return jnp.concatenate([order[...]] * lanes, axis=1) < here

    def key_rows(kt):
        return kvs[pl.ds(pl.multiple_of(kt * KEY_TILE, KEY_TILE), KEY_TILE), :]

    def weigh(kt, m):
        kt, m = jnp.minimum(kt, key_tiles - 1), jnp.minimum(m, row_blocks - 1)
        scores = jnp.dot(key_rows(kt), query_rows(m), preferred_element_type=jnp.float32)
        p = jnp.where(allowed_keys(m, kt), jnp.exp2(scores * TO_LOG2), 0.0)
        return p.astype(jnp.bfloat16)

    def fold(kt, m, p):
        kt = jnp.minimum(kt, key_tiles - 1)
        acc[m] = acc[m] + jnp.dot(vt[kt], p, preferred_element_type=jnp.float32)

    def advance(kt, m):
        wrap = m + 1 >= row_blocks
        kt = kt + wrap.astype(jnp.int32)
        return kt, jnp.where(wrap, lows[kt], m + 1)

    def body(_, carry):
        kt, m, flat = carry
        pairs = []
        for i in range(UNROLL):
            pairs.append((kt, m))
            kt, m = advance(kt, m)
        for i in range(UNROLL):
            fold(flat[2 * i], flat[2 * i + 1], probs[i])
            probs[i] = weigh(*pairs[i])
        return kt, m, tuple(v for pair in pairs for v in pair)

    nothing = (jnp.int32(0), jnp.int32(row_blocks)) * UNROLL
    steps = (total + UNROLL - 1) // UNROLL + 1
    lax.fori_loop(0, steps, body, (jnp.int32(0), lows[0], nothing))

    chunks = sems.shape[0]
    per_chunk = row_blocks // chunks

    def finish(m, worst):
        totals = acc[m, HEAD_DIM : HEAD_DIM + 1, :]
        staged[m] = (acc[m, :HEAD_DIM, :] * (1.0 / totals)).astype(jnp.bfloat16)
        fine = jnp.logical_and(totals > LEAST_TOTAL, totals < MOST_TOTAL)
        return jnp.maximum(worst, jnp.where(fine, 0.0, 1.0))

    def send(c):
        cut = pl.ds(c * per_chunk, per_chunk)
        return pltpu.make_async_copy(staged.at[cut], out_ref.at[cut], sems.at[c])

    worst = jnp.zeros((1, BLOCK_ROWS), jnp.float32)
    for c in range(chunks):
        worst = lax.fori_loop(c * per_chunk, (c + 1) * per_chunk, finish, worst)
        send(c).start()
    flag[0] = jnp.max(worst)
    for c in range(chunks):
        send(c).wait()

    @pl.when(flag[0] > 0.0)
    def _():
        def redo(m, carry):
            def masked_scores(kt):
                scores = jnp.dot(key_rows(kt), query_rows(m), preferred_element_type=jnp.float32)
                return scores * SCALE, allowed_keys(m, kt)

            def fold_max(kt, peak):
                scores, allowed = masked_scores(kt)
                masked = jnp.where(allowed, scores, -3e38)
                return jnp.maximum(peak, jnp.max(masked, axis=0, keepdims=True))

            peak = lax.fori_loop(
                0, key_tiles, fold_max, jnp.full((1, BLOCK_ROWS), -3e38, jnp.float32)
            )
            acc[m] = jnp.zeros(acc.shape[1:], jnp.float32)

            def fold_sum(kt, inner):
                scores, allowed = masked_scores(kt)
                p = jnp.where(allowed, jnp.exp(jnp.where(allowed, scores - peak, 0.0)), 0.0)
                fold(kt, m, p.astype(jnp.bfloat16))
                return inner

            lax.fori_loop(0, key_tiles, fold_sum, 0)
            totals = acc[m, HEAD_DIM : HEAD_DIM + 1, :]
            staged[m] = (acc[m, :HEAD_DIM, :] * (1.0 / totals)).astype(jnp.bfloat16)
            return carry

        lax.fori_loop(0, row_blocks, redo, 0)
        for c in range(chunks):
            send(c).start()
        for c in range(chunks):
            send(c).wait()


def attend_call(group, starts, counts, arrived, blocks):
    row_blocks = arrived.shape[0]
    patches = row_blocks * 128
    key_tiles = patches // KEY_TILE
    return pl.pallas_call(
        functools.partial(attend_kernel, blocks),
        out_shape=jax.ShapeDtypeStruct((row_blocks, HEAD_DIM, BLOCK_ROWS), jnp.bfloat16),
        in_specs=[smem(), smem(), vmem(), vmem()],
        out_specs=hbm(),
        scratch_shapes=[
            pltpu.VMEM((patches, 128), jnp.bfloat16),
            pltpu.VMEM((key_tiles, HEAD_DIM + SUM_ROWS, KEY_TILE), jnp.bfloat16),
            pltpu.VMEM((KEY_TILE, 128), jnp.int32),
            pltpu.VMEM((row_blocks + 1, HEAD_DIM + SUM_ROWS, BLOCK_ROWS), jnp.float32),
            pltpu.VMEM((UNROLL, KEY_TILE, BLOCK_ROWS), jnp.bfloat16),
            pltpu.VMEM((row_blocks, HEAD_DIM, BLOCK_ROWS), jnp.bfloat16),
            pltpu.SMEM((key_tiles + 2 * UNROLL + 2,), jnp.int32),
            pltpu.SMEM((1,), jnp.float32),
            pltpu.SemaphoreType.DMA((4,)),
        ],
        compiler_params=pltpu.CompilerParams(vmem_limit_bytes=50 * MIB),
        cost_estimate=pl.CostEstimate(
            flops=2 * patches * row_blocks * BLOCK_ROWS * 2 * HEAD_DIM,
            bytes_accessed=2 * 3 * arrived.size // 2,
            transcendentals=patches * row_blocks * BLOCK_ROWS // 2,
        ),
        name="attend",
    )(group, starts, counts, arrived)


OUT_PARTS = 4


def out_kernel(h_ref, w_ref, x_ref, gain_ref, out_ref, weights, acc, staged, ins, outs):
    copies = h_ref.shape[0]
    width = w_ref.shape[0]
    depth = width // OUT_PARTS
    loads = []
    for i in range(OUT_PARTS):
        cut = pl.ds(i * depth, depth)
        loads.append(pltpu.make_async_copy(w_ref.at[cut], weights.at[cut], ins.at[i]))
        loads[i].start()
    for i in range(OUT_PARTS):
        loads[i].wait()
        part = weights[i * depth : (i + 1) * depth, :]
        heads = depth // HEAD_DIM
        for r in range(copies):
            head_out = h_ref[r, i * heads : (i + 1) * heads].reshape(depth, BLOCK_ROWS).T
            product = jnp.dot(head_out, part, preferred_element_type=jnp.float32)
            acc[r] = product if i == 0 else acc[r] + product
    sent = []
    for r in range(copies):
        cut = slice(r * BLOCK_ROWS, (r + 1) * BLOCK_ROWS)
        residual = x_ref[cut, :].astype(jnp.float32) + acc[r]
        staged[cut, :] = norm_rows(residual, gain_ref[...]).astype(jnp.bfloat16)
        where = pl.ds(r * BLOCK_ROWS, BLOCK_ROWS)
        send = pltpu.make_async_copy(staged.at[where], out_ref.at[where], outs.at[r])
        send.start()
        sent.append(send)
    for send in sent:
        send.wait()


def out_call(head_out, w_out, x, gain):
    rows, width = x.shape
    return pl.pallas_call(
        out_kernel,
        out_shape=jax.ShapeDtypeStruct(x.shape, jnp.bfloat16),
        in_specs=[vmem(), hbm(), vmem(), vmem()],
        out_specs=hbm(),
        scratch_shapes=[
            pltpu.VMEM(w_out.shape, jnp.bfloat16),
            pltpu.VMEM((rows // BLOCK_ROWS, BLOCK_ROWS, width), jnp.float32),
            pltpu.VMEM(x.shape, jnp.bfloat16),
            pltpu.SemaphoreType.DMA((OUT_PARTS,)),
            pltpu.SemaphoreType.DMA((rows // BLOCK_ROWS,)),
        ],
        compiler_params=pltpu.CompilerParams(vmem_limit_bytes=50 * MIB),
        cost_estimate=pl.CostEstimate(
            flops=2 * rows * width * width, bytes_accessed=2 * (3 * rows * width + width * width),
            transcendentals=rows,
        ),
        name="outputs",
    )(head_out, w_out, x, gain.reshape(1, -1))


def per_device(
    byte_states, patch_latents, patch_lengths, w_down, kv_gain, w_query, w_key, w_value, w_out,
    out_gain,
):
    seqs, mps = lax.axis_size("seq"), lax.axis_size("mp")
    copies = mps // HEADS
    x = byte_states[0]
    patches_here, features = patch_latents.shape[1:]
    part = patches_here // mps

    sent = patch_latents.reshape(seqs * mps, part, features)
    latents = lax.all_to_all(sent, ("seq", "mp"), 0, 0, tiled=True)
    latents = latents.reshape(seqs, mps, part, features)
    lengths = patch_lengths[0].reshape(-1, 128)
    buf, starts, counts = query_call(x, w_query, lengths, mps * x.shape[0])

    buf = kv_call(latents, w_down, kv_gain, w_key, w_value, buf)
    arrived = lax.all_to_all(buf, "mp", 0, 0, tiled=True)

    group = jnp.stack([lax.axis_index("mp") // HEADS, jnp.int32(copies)])
    head_out = attend_call(group, starts, counts, arrived, seqs)
    head_out = lax.all_to_all(head_out, "mp", 0, 0, tiled=True)
    decoded = out_call(
        head_out.reshape(copies, HEADS, HEAD_DIM, BLOCK_ROWS), w_out, x, out_gain
    )
    return decoded[None]


def solution(mesh):
    return jax.shard_map(
        per_device,
        mesh=mesh,
        in_specs=(
            P("seq", "mp", None),
            P(None, "seq", "mp"),
            P("seq", None),
            P(),
            P(),
            P(),
            P(),
            P(),
            P(),
            P(),
        ),
        out_specs=P("seq", "mp", None),
        check_vma=False,
    )
```

```python
import functools
import math

import jax
import jax.numpy as jnp
from jax import lax
from jax.experimental import pallas as pl
from jax.experimental.pallas import tpu as pltpu
from jax.sharding import PartitionSpec as P

HEADS = 16
HEAD_DIM = 64
BLOCK_ROWS = 256
KEY_TILE = 512
UNROLL = 6
SUM_ROWS = 16
TO_LOG2 = math.log2(math.e) / math.sqrt(HEAD_DIM)
SCALE = 1.0 / math.sqrt(HEAD_DIM)
LEAST_TOTAL = 2.0**-90
MOST_TOTAL = 2.0**110
MIB = 1024 * 1024


def vmem():
    return pl.BlockSpec(memory_space=pltpu.VMEM)


def smem():
    return pl.BlockSpec(memory_space=pltpu.SMEM)


def hbm():
    return pl.BlockSpec(memory_space=pltpu.HBM)


def ones_where(mask):
    return mask.astype(jnp.float32).astype(jnp.bfloat16)


def iota(shape, dim):
    return lax.broadcasted_iota(jnp.int32, shape, dim)


def exact_dot(a, b):
    return jnp.dot(a, b, preferred_element_type=jnp.float32)


def patch_tables(lengths, starts_ref, counts_ref):
    lines, lanes = lengths.shape
    values = lengths.astype(jnp.float32).astype(jnp.bfloat16)
    square = (lanes, lanes)
    within = exact_dot(values, ones_where(iota(square, 0) < iota(square, 1)))
    small = (lines, lines)
    above = exact_dot(ones_where(iota(small, 1) < iota(small, 0)), values)
    starts = (within + jnp.sum(above, axis=1, keepdims=True)).astype(jnp.int32)
    starts_ref[...] = starts
    spots = counts_ref.shape[0]
    tops, lows = [], []
    for line in range(lines):
        row = starts[line : line + 1, :]
        tops.append(ones_where(iota((spots, lanes), 0) == lax.shift_right_logical(row, 7)))
        lows.append(ones_where(iota((128, lanes), 0) == jnp.bitwise_and(row, 127)))
    present = lax.dot_general(
        jnp.concatenate(tops, axis=1),
        jnp.concatenate(lows, axis=1),
        (((1,), (1,)), ((), ())),
        preferred_element_type=jnp.float32,
    ).astype(jnp.bfloat16)
    along = exact_dot(present, ones_where(iota((128, 128), 0) <= iota((128, 128), 1)))
    before = exact_dot(ones_where(iota((spots, spots), 1) < iota((spots, spots), 0)), present)
    counts_ref[...] = (along + jnp.sum(before, axis=1, keepdims=True)).astype(jnp.int32)


def query_kernel(x_ref, w_ref, len_ref, buf_ref, starts_ref, counts_ref, staged, sems):
    rows, width = x_ref.shape
    step = 256
    heads_step = step // HEAD_DIM
    copies = rows // BLOCK_ROWS
    half = BLOCK_ROWS // 128
    sent = []
    for n in range(width // step):
        q = jnp.dot(
            x_ref[...], w_ref[:, n * step : (n + 1) * step], preferred_element_type=jnp.float32
        ).astype(jnp.bfloat16)
        qt = q.T
        for r in range(copies):
            for h in range(heads_step):
                for b in range(half):
                    at = r * BLOCK_ROWS + b * 128
                    staged[r, n * heads_step + h, b * HEAD_DIM : (b + 1) * HEAD_DIM, :] = qt[
                        h * HEAD_DIM : (h + 1) * HEAD_DIM, at : at + 128
                    ]
            cut = pl.ds(n * heads_step, heads_step)
            send = pltpu.make_async_copy(
                staged.at[r, cut],
                buf_ref.at[pl.ds(r * HEADS + n * heads_step, heads_step), pl.ds(128, 128)],
                sems.at[n * copies + r],
            )
            send.start()
            sent.append(send)
    patch_tables(len_ref[...], starts_ref, counts_ref)
    for send in sent:
        send.wait()


def query_call(x, w_query, lengths, seq_len):
    rows, width = x.shape
    copies = rows // BLOCK_ROWS
    return pl.pallas_call(
        query_kernel,
        out_shape=(
            jax.ShapeDtypeStruct((copies * HEADS, 256, 128), jnp.bfloat16),
            jax.ShapeDtypeStruct(lengths.shape, jnp.int32),
            jax.ShapeDtypeStruct((seq_len // 128, 128), jnp.int32),
        ),
        in_specs=[vmem(), vmem(), vmem()],
        out_specs=(hbm(), vmem(), vmem()),
        scratch_shapes=[
            pltpu.VMEM((copies, HEADS, 128, 128), jnp.bfloat16),
            pltpu.SemaphoreType.DMA((copies * width // 256,)),
        ],
        compiler_params=pltpu.CompilerParams(vmem_limit_bytes=16 * MIB),
        cost_estimate=pl.CostEstimate(
            flops=2 * rows * width * width, bytes_accessed=2 * (2 * rows * width + width * width),
            transcendentals=0,
        ),
        name="queries",
    )(x, w_query, lengths)


def norm_rows(values, gain):
    mean_square = jnp.mean(values * values, axis=-1, keepdims=True)
    return values * lax.rsqrt(mean_square + 1e-05) * gain.astype(jnp.float32)


WD_PARTS = 8
AHEAD = 5


def kv_kernel(
    x_ref, wd_ref, gain_ref, wk_ref, wv_ref, old_ref, buf_ref, wd, wk, wv, acc, staged, sems, outs
):
    blocks, groups, part, lanes = x_ref.shape
    rows = blocks * part
    depth = wd_ref.shape[0] // WD_PARTS
    per_part = groups // WD_PARTS
    loads = [
        pltpu.make_async_copy(
            wd_ref.at[pl.ds(i * depth, depth)], wd.at[pl.ds(i * depth, depth)], sems.at[i]
        )
        for i in range(WD_PARTS)
    ]
    loads.append(pltpu.make_async_copy(wk_ref, wk, sems.at[WD_PARTS]))
    loads.append(pltpu.make_async_copy(wv_ref, wv, sems.at[WD_PARTS + 1]))
    for load in loads[:AHEAD]:
        load.start()
    for i in range(WD_PARTS):
        if i + AHEAD < len(loads):
            loads[i + AHEAD].start()
        lhs = jnp.concatenate(
            [x_ref[:, i * per_part + g].reshape(rows, lanes) for g in range(per_part)], axis=1
        )
        loads[i].wait()
        product = jnp.dot(
            lhs, wd[i * depth : (i + 1) * depth, :], preferred_element_type=jnp.float32
        )
        acc[...] = product if i == 0 else acc[...] + product
    for load in loads[WD_PARTS + AHEAD :]:
        load.start()
    normed = norm_rows(acc[...], gain_ref[...]).astype(jnp.bfloat16)
    loads[WD_PARTS].wait()
    loads[WD_PARTS + 1].wait()
    copies = buf_ref.shape[0] // HEADS
    step = 256
    heads_step = step // HEAD_DIM
    sent = []
    for n in range(wk.shape[1] // step):
        cut = slice(n * step, (n + 1) * step)
        keys = jnp.dot(normed, wk[:, cut], preferred_element_type=jnp.float32)
        values = jnp.dot(normed, wv[:, cut], preferred_element_type=jnp.float32)
        for h in range(heads_step):
            own = slice(h * HEAD_DIM, (h + 1) * HEAD_DIM)
            staged[n * heads_step + h] = jnp.concatenate(
                [keys[:, own], values[:, own]], axis=1
            ).astype(jnp.bfloat16)
        for r in range(copies):
            send = pltpu.make_async_copy(
                staged.at[pl.ds(n * heads_step, heads_step)],
                buf_ref.at[pl.ds(r * HEADS + n * heads_step, heads_step), pl.ds(0, 128)],
                outs.at[n * copies + r],
            )
            send.start()
            sent.append(send)
    for send in sent:
        send.wait()


def kv_call(x, w_down, gain, w_key, w_value, buf):
    blocks, groups, part, lanes = x.shape
    rows = blocks * part
    width = w_down.shape[1]
    return pl.pallas_call(
        kv_kernel,
        out_shape=jax.ShapeDtypeStruct(buf.shape, buf.dtype),
        in_specs=[vmem(), hbm(), vmem(), hbm(), hbm(), hbm()],
        out_specs=hbm(),
        input_output_aliases={5: 0},
        scratch_shapes=[
            pltpu.VMEM(w_down.shape, jnp.bfloat16),
            pltpu.VMEM(w_key.shape, jnp.bfloat16),
            pltpu.VMEM(w_value.shape, jnp.bfloat16),
            pltpu.VMEM((rows, width), jnp.float32),
            pltpu.VMEM((HEADS, rows, 2 * HEAD_DIM), jnp.bfloat16),
            pltpu.SemaphoreType.DMA((WD_PARTS + 2,)),
            pltpu.SemaphoreType.DMA((buf.shape[0] // HEADS * width // 256,)),
        ],
        compiler_params=pltpu.CompilerParams(vmem_limit_bytes=50 * MIB),
        cost_estimate=pl.CostEstimate(
            flops=2 * rows * width * (groups * lanes + 2 * width),
            bytes_accessed=2 * (rows * groups * lanes + groups * lanes * width + 2 * width * width),
            transcendentals=0,
        ),
        name="keys_values",
    )(x, w_down, gain.reshape(1, -1), w_key, w_value, buf)


def stage(rhs, register, mxu):
    pltpu.matmul_push_rhs(rhs, staging_register=register, mxu_index=mxu)


def attend_kernel(blocks, *refs):
    unit = KEY_TILE // 2
    kinds = []
    for mxu in range(2):
        kinds += [pltpu.ACC(mxu)((unit, BLOCK_ROWS), jnp.float32)] * 3
        kinds += [pltpu.ACC(mxu)((HEAD_DIM + SUM_ROWS, BLOCK_ROWS), jnp.float32)] * 3
    pl.run_scoped(functools.partial(attend_body, blocks, refs), *kinds)


def attend_body(blocks, refs, *accs):
    group_ref, starts_ref, counts_ref, in_ref, out_ref = refs[:5]
    kvs, vt, order, acc, probs, staged, split, lows, flag, sems = refs[5:]
    score_accs, sum_accs = (accs[0:3], accs[6:9]), (accs[3:6], accs[9:12])
    unit = KEY_TILE // 2
    row_blocks = in_ref.shape[0]
    senders = row_blocks
    part = 128 // blocks
    patches = kvs.shape[0]
    key_tiles = patches // KEY_TILE
    stride = BLOCK_ROWS * group_ref[1]
    group = group_ref[0]

    def ceil_blocks(rows):
        return jnp.minimum((jnp.maximum(rows, 0) + stride - 1) // stride, row_blocks)

    total = jnp.int32(0)
    for kt in range(lows.shape[0]):
        if kt < key_tiles:
            start = starts_ref[kt * KEY_TILE // 128, 0]
            low = ceil_blocks(start - group * BLOCK_ROWS - (BLOCK_ROWS - 1))
            total = total + row_blocks - low
        else:
            low = jnp.int32(row_blocks)
        lows[kt] = low

    for b in range(blocks):
        for s in range(senders):
            at = (b * senders + s) * part
            kvs[at : at + part, :] = in_ref[s, b * part : (b + 1) * part, :]
    sum_row = ones_where(iota((SUM_ROWS, KEY_TILE), 0) == 0)
    for t in range(key_tiles):
        turned = kvs[t * KEY_TILE : (t + 1) * KEY_TILE, :].T
        vt[t, :HEAD_DIM, :] = turned[HEAD_DIM:, :]
        vt[t, HEAD_DIM:, :] = sum_row
        own = kvs[t * KEY_TILE : (t + 1) * KEY_TILE, :HEAD_DIM]
        kvs[t * KEY_TILE : (t + 1) * KEY_TILE, :] = jnp.concatenate([own, own], axis=1)
    order[...] = iota(order.shape, 0).astype(jnp.float32).astype(jnp.bfloat16)

    blank = jnp.zeros((unit, 128), jnp.bfloat16)
    lanes = BLOCK_ROWS // 128

    def prepare(m, carry):
        halves = [
            in_ref[m, 128 + b * HEAD_DIM : 128 + (b + 1) * HEAD_DIM, :] for b in range(lanes)
        ]
        scaled = jnp.concatenate(halves, axis=1).astype(jnp.float32) * TO_LOG2
        high = scaled.astype(jnp.bfloat16)
        split[m, :HEAD_DIM, :] = high
        split[m, HEAD_DIM:, :] = (scaled - high.astype(jnp.float32)).astype(jnp.bfloat16)
        acc[m] = jnp.zeros(acc.shape[1:], jnp.float32)
        return carry

    lax.fori_loop(0, row_blocks, prepare, 0)
    acc[row_blocks] = jnp.zeros(acc.shape[1:], jnp.float32)

    def query_rows(m):
        return jnp.concatenate([split[m], jnp.zeros((128, BLOCK_ROWS), jnp.bfloat16)], axis=0)

    def exact_query_rows(m):
        halves = [
            in_ref[m, 128 + b * HEAD_DIM : 128 + (b + 1) * HEAD_DIM, :] for b in range(lanes)
        ]
        zeros = jnp.zeros((256 - HEAD_DIM, BLOCK_ROWS), jnp.bfloat16)
        return jnp.concatenate([jnp.concatenate(halves, axis=1), zeros], axis=0)

    def last_keys(m):
        line = (m * stride + group * BLOCK_ROWS) // 128
        met = [counts_ref[pl.ds(line + b, 1), :] for b in range(lanes)]
        return jnp.concatenate(met, axis=1)

    def allowed_keys(m, kt, part):
        met = jnp.clip(last_keys(m) - (kt * KEY_TILE + part * unit), 0, unit)
        met = met.astype(jnp.float32).astype(jnp.bfloat16)
        return jnp.concatenate([order[...]] * lanes, axis=1) < met

    def key_rows(kt, part):
        at = pl.multiple_of(kt * KEY_TILE + part * unit, unit)
        return jnp.concatenate([kvs[pl.ds(at, unit), :], blank], axis=1)

    def value_columns(kt, part):
        return vt[kt, :, part * unit : (part + 1) * unit]

    def inside(kt, m):
        return jnp.minimum(kt, key_tiles - 1), jnp.minimum(m, row_blocks - 1)

    def advance(kt, m):
        wrap = m + 1 >= row_blocks
        kt = kt + wrap.astype(jnp.int32)
        return kt, jnp.where(wrap, lows[kt], m + 1)

    def ring(i, part):
        return score_accs[i % 2][(2 * (i // 2) + part) % 3]

    def total_of(i):
        return sum_accs[i % 2][(i // 2) % 3]

    def settle_scores(i, part, kt, m):
        p = jnp.exp2(pltpu.matmul_pop(ring(i, part))).astype(jnp.bfloat16)
        p = jnp.where(allowed_keys(m, kt, part), p, jnp.zeros_like(p))
        probs[i, part * unit : (part + 1) * unit] = p

    def settle_sums(i, m):
        acc[m] = acc[m] + pltpu.matmul_pop(total_of(i))

    def stage_first(kt, m):
        for mxu in range(2):
            stage(query_rows(inside(kt, m)[1]), 0, mxu)
            kt, m = advance(kt, m)

    def body(_, carry):
        kt, m, old, open_sums = carry
        pairs = []
        for i in range(UNROLL):
            pairs.append(inside(kt, m) + (m,))
            kt, m = advance(kt, m)
        for j in range(0, UNROLL, 2):
            now = (j, j + 1)
            if j == 0:
                before = [
                    (i, old[3 * i], old[3 * i + 1], open_sums[i - UNROLL + 2])
                    for i in (UNROLL - 2, UNROLL - 1)
                ]
            else:
                before = [(i, pairs[i][0], pairs[i][1], old[3 * i + 2]) for i in (j - 2, j - 1)]
            for i in now:
                pltpu.matmul_acc_lhs(ring(i, 0), key_rows(pairs[i][0], 0), load_staged_rhs=0)
                stage(probs[i, :unit], 0, i % 2)
                stage(probs[i, unit:], 1, i % 2)
            for i, b_kt, b_m, _ in before:
                settle_scores(i, 0, b_kt, b_m)
            for i in now:
                pltpu.matmul_acc_lhs(ring(i, 1), key_rows(pairs[i][0], 1))
            for i, b_kt, b_m, _ in before:
                settle_scores(i, 1, b_kt, b_m)
            for i in now:
                old_kt = old[3 * i]
                pltpu.matmul_acc_lhs(total_of(i), value_columns(old_kt, 0), load_staged_rhs=0)
                if i + 2 < UNROLL:
                    stage(query_rows(pairs[i + 2][1]), 0, i % 2)
                pltpu.matmul_acc_lhs(total_of(i), value_columns(old_kt, 1), load_staged_rhs=1)
            for i, _, _, b_m in before:
                settle_sums(i, b_m)
        stage_first(kt, m)
        now_open = tuple(old[3 * i + 2] for i in (UNROLL - 2, UNROLL - 1))
        return kt, m, tuple(v for pair in pairs for v in pair), now_open

    trash = jnp.int32(row_blocks)
    nothing = (jnp.int32(0), jnp.int32(0), trash) * UNROLL
    steps = (total + UNROLL - 1) // UNROLL + 1
    for spare in accs:
        probs[0, : spare.shape[0]] = pltpu.matmul_pop(spare).astype(jnp.bfloat16)
    first = (jnp.int32(0), lows[0])
    stage_first(*first)
    kt, m, _, open_sums = lax.fori_loop(0, steps, body, first + (nothing, (trash, trash)))
    for i in (UNROLL - 2, UNROLL - 1):
        settle_sums(i, open_sums[i - UNROLL + 2])
        for part in range(2):
            probs[i, part * unit : (part + 1) * unit] = pltpu.matmul_pop(ring(i, part)).astype(
                jnp.bfloat16
            )
        pltpu.matmul_acc_lhs(ring(i, 0), jnp.zeros((unit, 256), jnp.bfloat16), load_staged_rhs=0)
        probs[i, :unit] = pltpu.matmul_pop(ring(i, 0)).astype(jnp.bfloat16)

    chunks = sems.shape[0]
    per_chunk = row_blocks // chunks

    def finish(m, worst):
        totals = acc[m, HEAD_DIM : HEAD_DIM + 1, :]
        staged[m] = (acc[m, :HEAD_DIM, :] * (1.0 / totals)).astype(jnp.bfloat16)
        fine = jnp.logical_and(totals > LEAST_TOTAL, totals < MOST_TOTAL)
        return jnp.maximum(worst, jnp.where(fine, 0.0, 1.0))

    def send(c):
        cut = pl.ds(c * per_chunk, per_chunk)
        return pltpu.make_async_copy(staged.at[cut], out_ref.at[cut], sems.at[c])

    worst = jnp.zeros((1, BLOCK_ROWS), jnp.float32)
    for c in range(chunks):
        worst = lax.fori_loop(c * per_chunk, (c + 1) * per_chunk, finish, worst)
        send(c).start()
    flag[0] = jnp.max(worst)
    for c in range(chunks):
        send(c).wait()

    @pl.when(flag[0] > 0.0)
    def _():
        def redo(m, carry):
            def masked_scores(kt):
                stage(exact_query_rows(m), 0, 0)
                pltpu.matmul_acc_lhs(score_accs[0][0], key_rows(kt, 0), load_staged_rhs=0)
                pltpu.matmul_acc_lhs(score_accs[0][1], key_rows(kt, 1))
                parts = []
                for part in range(2):
                    scores = pltpu.matmul_pop(score_accs[0][part]) * SCALE
                    met = jnp.clip(last_keys(m) - (kt * KEY_TILE + part * unit), 0, unit)
                    parts.append((scores, iota((unit, BLOCK_ROWS), 0) < met))
                return parts

            def fold_max(kt, peak):
                for scores, allowed in masked_scores(kt):
                    masked = jnp.where(allowed, scores, -3e38)
                    peak = jnp.maximum(peak, jnp.max(masked, axis=0, keepdims=True))
                return peak

            peak = lax.fori_loop(
                0, key_tiles, fold_max, jnp.full((1, BLOCK_ROWS), -3e38, jnp.float32)
            )
            acc[m] = jnp.zeros(acc.shape[1:], jnp.float32)

            def fold_sum(kt, inner):
                for part, (scores, allowed) in enumerate(masked_scores(kt)):
                    p = jnp.where(allowed, jnp.exp(jnp.where(allowed, scores - peak, 0.0)), 0.0)
                    stage(p.astype(jnp.bfloat16), 0, 0)
                    pltpu.matmul_acc_lhs(
                        sum_accs[0][0], value_columns(kt, part), load_staged_rhs=0
                    )
                acc[m] = acc[m] + pltpu.matmul_pop(sum_accs[0][0])
                return inner

            lax.fori_loop(0, key_tiles, fold_sum, 0)
            totals = acc[m, HEAD_DIM : HEAD_DIM + 1, :]
            staged[m] = (acc[m, :HEAD_DIM, :] * (1.0 / totals)).astype(jnp.bfloat16)
            return carry

        lax.fori_loop(0, row_blocks, redo, 0)
        for c in range(chunks):
            send(c).start()
        for c in range(chunks):
            send(c).wait()


def attend_call(group, starts, counts, arrived, blocks):
    row_blocks = arrived.shape[0]
    patches = row_blocks * 128
    key_tiles = patches // KEY_TILE
    return pl.pallas_call(
        functools.partial(attend_kernel, blocks),
        out_shape=jax.ShapeDtypeStruct((row_blocks, HEAD_DIM, BLOCK_ROWS), jnp.bfloat16),
        in_specs=[smem(), smem(), vmem(), vmem()],
        out_specs=hbm(),
        scratch_shapes=[
            pltpu.VMEM((patches, 128), jnp.bfloat16),
            pltpu.VMEM((key_tiles, HEAD_DIM + SUM_ROWS, KEY_TILE), jnp.bfloat16),
            pltpu.VMEM((KEY_TILE // 2, 128), jnp.bfloat16),
            pltpu.VMEM((row_blocks + 1, HEAD_DIM + SUM_ROWS, BLOCK_ROWS), jnp.float32),
            pltpu.VMEM((UNROLL, KEY_TILE, BLOCK_ROWS), jnp.bfloat16),
            pltpu.VMEM((row_blocks, HEAD_DIM, BLOCK_ROWS), jnp.bfloat16),
            pltpu.VMEM((row_blocks, 2 * HEAD_DIM, BLOCK_ROWS), jnp.bfloat16),
            pltpu.SMEM((key_tiles + 2 * UNROLL + 2,), jnp.int32),
            pltpu.SMEM((1,), jnp.float32),
            pltpu.SemaphoreType.DMA((4,)),
        ],
        compiler_params=pltpu.CompilerParams(vmem_limit_bytes=50 * MIB),
        cost_estimate=pl.CostEstimate(
            flops=2 * patches * row_blocks * BLOCK_ROWS * 2 * HEAD_DIM,
            bytes_accessed=2 * 3 * arrived.size // 2,
            transcendentals=patches * row_blocks * BLOCK_ROWS // 2,
        ),
        name="attend",
    )(group, starts, counts, arrived)


OUT_PARTS = 4


def out_kernel(h_ref, w_ref, x_ref, gain_ref, out_ref, weights, acc, staged, ins, outs):
    copies = h_ref.shape[0]
    width = w_ref.shape[0]
    depth = width // OUT_PARTS
    loads = []
    for i in range(OUT_PARTS):
        cut = pl.ds(i * depth, depth)
        loads.append(pltpu.make_async_copy(w_ref.at[cut], weights.at[cut], ins.at[i]))
        loads[i].start()
    for i in range(OUT_PARTS):
        loads[i].wait()
        part = weights[i * depth : (i + 1) * depth, :]
        heads = depth // HEAD_DIM
        for r in range(copies):
            head_out = h_ref[r, i * heads : (i + 1) * heads].reshape(depth, BLOCK_ROWS).T
            product = jnp.dot(head_out, part, preferred_element_type=jnp.float32)
            acc[r] = product if i == 0 else acc[r] + product
    sent = []
    for r in range(copies):
        cut = slice(r * BLOCK_ROWS, (r + 1) * BLOCK_ROWS)
        residual = x_ref[cut, :].astype(jnp.float32) + acc[r]
        staged[cut, :] = norm_rows(residual, gain_ref[...]).astype(jnp.bfloat16)
        where = pl.ds(r * BLOCK_ROWS, BLOCK_ROWS)
        send = pltpu.make_async_copy(staged.at[where], out_ref.at[where], outs.at[r])
        send.start()
        sent.append(send)
    for send in sent:
        send.wait()


def out_call(head_out, w_out, x, gain):
    rows, width = x.shape
    return pl.pallas_call(
        out_kernel,
        out_shape=jax.ShapeDtypeStruct(x.shape, jnp.bfloat16),
        in_specs=[vmem(), hbm(), vmem(), vmem()],
        out_specs=hbm(),
        scratch_shapes=[
            pltpu.VMEM(w_out.shape, jnp.bfloat16),
            pltpu.VMEM((rows // BLOCK_ROWS, BLOCK_ROWS, width), jnp.float32),
            pltpu.VMEM(x.shape, jnp.bfloat16),
            pltpu.SemaphoreType.DMA((OUT_PARTS,)),
            pltpu.SemaphoreType.DMA((rows // BLOCK_ROWS,)),
        ],
        compiler_params=pltpu.CompilerParams(vmem_limit_bytes=50 * MIB),
        cost_estimate=pl.CostEstimate(
            flops=2 * rows * width * width, bytes_accessed=2 * (3 * rows * width + width * width),
            transcendentals=rows,
        ),
        name="outputs",
    )(head_out, w_out, x, gain.reshape(1, -1))


def per_device(
    byte_states, patch_latents, patch_lengths, w_down, kv_gain, w_query, w_key, w_value, w_out,
    out_gain,
):
    seqs, mps = lax.axis_size("seq"), lax.axis_size("mp")
    copies = mps // HEADS
    x = byte_states[0]
    patches_here, features = patch_latents.shape[1:]
    part = patches_here // mps

    sent = patch_latents.reshape(seqs * mps, part, features)
    latents = lax.all_to_all(sent, ("seq", "mp"), 0, 0, tiled=True)
    latents = latents.reshape(seqs, mps, part, features)
    lengths = patch_lengths[0].reshape(-1, 128)
    buf, starts, counts = query_call(x, w_query, lengths, mps * x.shape[0])

    buf = kv_call(latents, w_down, kv_gain, w_key, w_value, buf)
    arrived = lax.all_to_all(buf, "mp", 0, 0, tiled=True)

    group = jnp.stack([lax.axis_index("mp") // HEADS, jnp.int32(copies)])
    head_out = attend_call(group, starts, counts, arrived, seqs)
    head_out = lax.all_to_all(head_out, "mp", 0, 0, tiled=True)
    decoded = out_call(
        head_out.reshape(copies, HEADS, HEAD_DIM, BLOCK_ROWS), w_out, x, out_gain
    )
    return decoded[None]


def solution(mesh):
    return jax.shard_map(
        per_device,
        mesh=mesh,
        in_specs=(
            P("seq", "mp", None),
            P(None, "seq", "mp"),
            P("seq", None),
            P(),
            P(),
            P(),
            P(),
            P(),
            P(),
            P(),
        ),
        out_specs=P("seq", "mp", None),
        check_vma=False,
    )
```

```python
import functools
import math

import jax
import jax.numpy as jnp
from jax import lax
from jax.experimental import pallas as pl
from jax.experimental.pallas import tpu as pltpu
from jax.sharding import PartitionSpec as P

HEADS = 16
HEAD_DIM = 64
BLOCK_ROWS = 256
KEY_TILE = 512
UNROLL = 6
SUM_ROWS = 16
TO_LOG2 = math.log2(math.e) / math.sqrt(HEAD_DIM)
SCALE = 1.0 / math.sqrt(HEAD_DIM)
LEAST_TOTAL = 2.0**-90
MOST_TOTAL = 2.0**110
MIB = 1024 * 1024


def vmem():
    return pl.BlockSpec(memory_space=pltpu.VMEM)


def smem():
    return pl.BlockSpec(memory_space=pltpu.SMEM)


def hbm():
    return pl.BlockSpec(memory_space=pltpu.HBM)


def ones_where(mask):
    return mask.astype(jnp.float32).astype(jnp.bfloat16)


def iota(shape, dim):
    return lax.broadcasted_iota(jnp.int32, shape, dim)


def exact_dot(a, b):
    return jnp.dot(a, b, preferred_element_type=jnp.float32)


def patch_tables(lengths, starts_ref, counts_ref):
    lines, lanes = lengths.shape
    values = lengths.astype(jnp.float32).astype(jnp.bfloat16)
    square = (lanes, lanes)
    within = exact_dot(values, ones_where(iota(square, 0) < iota(square, 1)))
    small = (lines, lines)
    above = exact_dot(ones_where(iota(small, 1) < iota(small, 0)), values)
    starts = (within + jnp.sum(above, axis=1, keepdims=True)).astype(jnp.int32)
    starts_ref[...] = starts
    spots = counts_ref.shape[0]
    tops, lows = [], []
    for line in range(lines):
        row = starts[line : line + 1, :]
        tops.append(ones_where(iota((spots, lanes), 0) == lax.shift_right_logical(row, 7)))
        lows.append(ones_where(iota((128, lanes), 0) == jnp.bitwise_and(row, 127)))
    present = lax.dot_general(
        jnp.concatenate(tops, axis=1),
        jnp.concatenate(lows, axis=1),
        (((1,), (1,)), ((), ())),
        preferred_element_type=jnp.float32,
    ).astype(jnp.bfloat16)
    along = exact_dot(present, ones_where(iota((128, 128), 0) <= iota((128, 128), 1)))
    before = exact_dot(ones_where(iota((spots, spots), 1) < iota((spots, spots), 0)), present)
    counts_ref[...] = (along + jnp.sum(before, axis=1, keepdims=True)).astype(jnp.int32)


def query_kernel(
    x_ref, w_ref, len_ref, buf_ref, starts_ref, counts_ref, kept_ref, staged, sems, keep_sem
):
    rows, width = x_ref.shape
    step = 256
    heads_step = step // HEAD_DIM
    copies = rows // BLOCK_ROWS
    half = BLOCK_ROWS // 128
    keep = pltpu.make_async_copy(x_ref, kept_ref, keep_sem.at[0])
    keep.start()
    sent = [keep]
    for n in range(width // step):
        q = jnp.dot(
            x_ref[...], w_ref[:, n * step : (n + 1) * step], preferred_element_type=jnp.float32
        ).astype(jnp.bfloat16)
        qt = q.T
        for r in range(copies):
            for h in range(heads_step):
                for b in range(half):
                    at = r * BLOCK_ROWS + b * 128
                    staged[r, n * heads_step + h, b * HEAD_DIM : (b + 1) * HEAD_DIM, :] = qt[
                        h * HEAD_DIM : (h + 1) * HEAD_DIM, at : at + 128
                    ]
            cut = pl.ds(n * heads_step, heads_step)
            send = pltpu.make_async_copy(
                staged.at[r, cut],
                buf_ref.at[pl.ds(r * HEADS + n * heads_step, heads_step), pl.ds(128, 128)],
                sems.at[n * copies + r],
            )
            send.start()
            sent.append(send)
    patch_tables(len_ref[...], starts_ref, counts_ref)
    for send in sent:
        send.wait()


def query_call(x, w_query, lengths, seq_len):
    rows, width = x.shape
    copies = rows // BLOCK_ROWS
    return pl.pallas_call(
        query_kernel,
        out_shape=(
            jax.ShapeDtypeStruct((copies * HEADS, 256, 128), jnp.bfloat16),
            jax.ShapeDtypeStruct(lengths.shape, jnp.int32),
            jax.ShapeDtypeStruct((seq_len // 128, 128), jnp.int32),
            jax.ShapeDtypeStruct(x.shape, x.dtype),
        ),
        in_specs=[vmem(), vmem(), vmem()],
        out_specs=(hbm(), vmem(), vmem(), hbm()),
        scratch_shapes=[
            pltpu.VMEM((copies, HEADS, 128, 128), jnp.bfloat16),
            pltpu.SemaphoreType.DMA((copies * width // 256,)),
            pltpu.SemaphoreType.DMA((1,)),
        ],
        compiler_params=pltpu.CompilerParams(vmem_limit_bytes=16 * MIB),
        cost_estimate=pl.CostEstimate(
            flops=2 * rows * width * width, bytes_accessed=2 * (2 * rows * width + width * width),
            transcendentals=0,
        ),
        name="queries",
    )(x, w_query, lengths)


def norm_rows(values, gain):
    mean_square = jnp.mean(values * values, axis=-1, keepdims=True)
    return values * lax.rsqrt(mean_square + 1e-05) * gain.astype(jnp.float32)


WD_PARTS = 8
AHEAD = 5


def kv_kernel(
    x_ref, wd_ref, gain_ref, wk_ref, wv_ref, old_ref, buf_ref, wd, wk, wv, acc, staged, sems, outs
):
    blocks, groups, part, lanes = x_ref.shape
    rows = blocks * part
    depth = wd_ref.shape[0] // WD_PARTS
    per_part = groups // WD_PARTS
    loads = [
        pltpu.make_async_copy(
            wd_ref.at[pl.ds(i * depth, depth)], wd.at[pl.ds(i * depth, depth)], sems.at[i]
        )
        for i in range(WD_PARTS)
    ]
    loads.append(pltpu.make_async_copy(wk_ref, wk, sems.at[WD_PARTS]))
    loads.append(pltpu.make_async_copy(wv_ref, wv, sems.at[WD_PARTS + 1]))
    for load in loads[:AHEAD]:
        load.start()
    for i in range(WD_PARTS):
        if i + AHEAD < len(loads):
            loads[i + AHEAD].start()
        lhs = jnp.concatenate(
            [x_ref[:, i * per_part + g].reshape(rows, lanes) for g in range(per_part)], axis=1
        )
        loads[i].wait()
        product = jnp.dot(
            lhs, wd[i * depth : (i + 1) * depth, :], preferred_element_type=jnp.float32
        )
        acc[...] = product if i == 0 else acc[...] + product
    for load in loads[WD_PARTS + AHEAD :]:
        load.start()
    normed = norm_rows(acc[...], gain_ref[...]).astype(jnp.bfloat16)
    copies = buf_ref.shape[0] // HEADS
    step = 256
    heads_step = step // HEAD_DIM
    loads[WD_PARTS].wait()
    acc[...] = jnp.dot(normed, wk[...], preferred_element_type=jnp.float32)
    loads[WD_PARTS + 1].wait()
    sent = []
    for n in range(wv.shape[1] // step):
        cut = slice(n * step, (n + 1) * step)
        keys = acc[:, cut]
        values = jnp.dot(normed, wv[:, cut], preferred_element_type=jnp.float32)
        for h in range(heads_step):
            own = slice(h * HEAD_DIM, (h + 1) * HEAD_DIM)
            staged[n * heads_step + h] = jnp.concatenate(
                [keys[:, own], values[:, own]], axis=1
            ).astype(jnp.bfloat16)
        for r in range(copies):
            send = pltpu.make_async_copy(
                staged.at[pl.ds(n * heads_step, heads_step)],
                buf_ref.at[pl.ds(r * HEADS + n * heads_step, heads_step), pl.ds(0, 128)],
                outs.at[n * copies + r],
            )
            send.start()
            sent.append(send)
    for send in sent:
        send.wait()


def kv_call(x, w_down, gain, w_key, w_value, buf):
    blocks, groups, part, lanes = x.shape
    rows = blocks * part
    width = w_down.shape[1]
    return pl.pallas_call(
        kv_kernel,
        out_shape=jax.ShapeDtypeStruct(buf.shape, buf.dtype),
        in_specs=[vmem(), hbm(), vmem(), hbm(), hbm(), hbm()],
        out_specs=hbm(),
        input_output_aliases={5: 0},
        scratch_shapes=[
            pltpu.VMEM(w_down.shape, jnp.bfloat16),
            pltpu.VMEM(w_key.shape, jnp.bfloat16),
            pltpu.VMEM(w_value.shape, jnp.bfloat16),
            pltpu.VMEM((rows, width), jnp.float32),
            pltpu.VMEM((HEADS, rows, 2 * HEAD_DIM), jnp.bfloat16),
            pltpu.SemaphoreType.DMA((WD_PARTS + 2,)),
            pltpu.SemaphoreType.DMA((buf.shape[0] // HEADS * width // 256,)),
        ],
        compiler_params=pltpu.CompilerParams(vmem_limit_bytes=50 * MIB),
        cost_estimate=pl.CostEstimate(
            flops=2 * rows * width * (groups * lanes + 2 * width),
            bytes_accessed=2 * (rows * groups * lanes + groups * lanes * width + 2 * width * width),
            transcendentals=0,
        ),
        name="keys_values",
    )(x, w_down, gain.reshape(1, -1), w_key, w_value, buf)


def stage(rhs, register, mxu):
    pltpu.matmul_push_rhs(rhs, staging_register=register, mxu_index=mxu)


def attend_kernel(blocks, *refs):
    unit = KEY_TILE // 2
    kinds = []
    for mxu in range(2):
        kinds += [pltpu.ACC(mxu)((unit, BLOCK_ROWS), jnp.float32)] * 3
        kinds += [pltpu.ACC(mxu)((HEAD_DIM + SUM_ROWS, BLOCK_ROWS), jnp.float32)] * 3
    pl.run_scoped(functools.partial(attend_body, blocks, refs), *kinds)


def attend_body(blocks, refs, *accs):
    group_ref, starts_ref, counts_ref, in_ref, out_ref = refs[:5]
    kvs, vt, order, acc, probs, split, lows, flag = refs[5:]
    score_accs, sum_accs = (accs[0:3], accs[6:9]), (accs[3:6], accs[9:12])
    unit = KEY_TILE // 2
    row_blocks = in_ref.shape[0]
    senders = row_blocks
    part = 128 // blocks
    patches = kvs.shape[0]
    key_tiles = patches // KEY_TILE
    stride = BLOCK_ROWS * group_ref[1]
    group = group_ref[0]

    def ceil_blocks(rows):
        return jnp.minimum((jnp.maximum(rows, 0) + stride - 1) // stride, row_blocks)

    total = jnp.int32(0)
    for kt in range(lows.shape[0]):
        if kt < key_tiles:
            start = starts_ref[kt * KEY_TILE // 128, 0]
            low = ceil_blocks(start - group * BLOCK_ROWS - (BLOCK_ROWS - 1))
            total = total + row_blocks - low
        else:
            low = jnp.int32(row_blocks)
        lows[kt] = low

    for b in range(blocks):
        for s in range(senders):
            at = (b * senders + s) * part
            kvs[at : at + part, :] = in_ref[s, b * part : (b + 1) * part, :]
    sum_row = ones_where(iota((SUM_ROWS, KEY_TILE), 0) == 0)
    for t in range(key_tiles):
        turned = kvs[t * KEY_TILE : (t + 1) * KEY_TILE, :].T
        vt[t, :HEAD_DIM, :] = turned[HEAD_DIM:, :]
        vt[t, HEAD_DIM:, :] = sum_row
    order[...] = iota(order.shape, 0).astype(jnp.float32).astype(jnp.bfloat16)

    lanes = BLOCK_ROWS // 128

    def prepare(m, carry):
        halves = [
            in_ref[m, 128 + b * HEAD_DIM : 128 + (b + 1) * HEAD_DIM, :] for b in range(lanes)
        ]
        scaled = jnp.concatenate(halves, axis=1).astype(jnp.float32) * TO_LOG2
        high = scaled.astype(jnp.bfloat16)
        split[m, :HEAD_DIM, :] = high
        split[m, HEAD_DIM:, :] = (scaled - high.astype(jnp.float32)).astype(jnp.bfloat16)
        acc[m] = jnp.zeros(acc.shape[1:], jnp.float32)
        return carry

    def four(step):
        def steps(i, carry):
            for k in range(4):
                carry = step(4 * i + k, carry)
            return carry

        return steps

    lax.fori_loop(0, row_blocks // 4, four(prepare), 0)
    acc[row_blocks] = jnp.zeros(acc.shape[1:], jnp.float32)

    def query_rows(m):
        gap = jnp.zeros((HEAD_DIM, BLOCK_ROWS), jnp.bfloat16)
        return jnp.concatenate([split[m, :HEAD_DIM, :], gap, split[m, HEAD_DIM:, :], gap], axis=0)

    def exact_query_rows(m):
        halves = [
            in_ref[m, 128 + b * HEAD_DIM : 128 + (b + 1) * HEAD_DIM, :] for b in range(lanes)
        ]
        zeros = jnp.zeros((256 - HEAD_DIM, BLOCK_ROWS), jnp.bfloat16)
        return jnp.concatenate([jnp.concatenate(halves, axis=1), zeros], axis=0)

    def last_keys(m):
        line = (m * stride + group * BLOCK_ROWS) // 128
        met = [counts_ref[pl.ds(line + b, 1), :] for b in range(lanes)]
        return jnp.concatenate(met, axis=1)

    def allowed_keys(m, kt, part):
        met = jnp.clip(last_keys(m) - (kt * KEY_TILE + part * unit), 0, unit)
        met = met.astype(jnp.float32).astype(jnp.bfloat16)
        return jnp.concatenate([order[...]] * lanes, axis=1) < met

    def key_rows(kt, part):
        at = pl.multiple_of(kt * KEY_TILE + part * unit, unit)
        return jnp.concatenate([kvs[pl.ds(at, unit), :]] * 2, axis=1)

    def value_columns(kt, part):
        return vt[kt, :, part * unit : (part + 1) * unit]

    def inside(kt, m):
        return jnp.minimum(kt, key_tiles - 1), jnp.minimum(m, row_blocks - 1)

    def advance(kt, m):
        wrap = m + 1 >= row_blocks
        kt = kt + wrap.astype(jnp.int32)
        return kt, jnp.where(wrap, lows[kt], m + 1)

    def ring(i, part):
        return score_accs[i % 2][(2 * (i // 2) + part) % 3]

    def total_of(i):
        return sum_accs[i % 2][(i // 2) % 3]

    def settle_scores(i, part, kt, m):
        p = jnp.exp2(pltpu.matmul_pop(ring(i, part))).astype(jnp.bfloat16)
        p = jnp.where(allowed_keys(m, kt, part), p, jnp.zeros_like(p))
        probs[i, part * unit : (part + 1) * unit] = p

    def settle_sums(i, m):
        acc[m] = acc[m] + pltpu.matmul_pop(total_of(i))

    def stage_first(kt, m):
        for mxu in range(2):
            stage(query_rows(inside(kt, m)[1]), 0, mxu)
            kt, m = advance(kt, m)

    def body(_, carry):
        kt, m, old, open_sums = carry
        pairs = []
        for i in range(UNROLL):
            pairs.append(inside(kt, m) + (m,))
            kt, m = advance(kt, m)
        for j in range(0, UNROLL, 2):
            now = (j, j + 1)
            if j == 0:
                before = [
                    (i, old[3 * i], old[3 * i + 1], open_sums[i - UNROLL + 2])
                    for i in (UNROLL - 2, UNROLL - 1)
                ]
            else:
                before = [(i, pairs[i][0], pairs[i][1], old[3 * i + 2]) for i in (j - 2, j - 1)]
            for i in now:
                pltpu.matmul_acc_lhs(ring(i, 0), key_rows(pairs[i][0], 0), load_staged_rhs=0)
                stage(probs[i, :unit], 0, i % 2)
                stage(probs[i, unit:], 1, i % 2)
            for i, b_kt, b_m, _ in before:
                settle_scores(i, 0, b_kt, b_m)
            for i in now:
                pltpu.matmul_acc_lhs(ring(i, 1), key_rows(pairs[i][0], 1))
            for i, b_kt, b_m, _ in before:
                settle_scores(i, 1, b_kt, b_m)
            for i in now:
                old_kt = old[3 * i]
                pltpu.matmul_acc_lhs(total_of(i), value_columns(old_kt, 0), load_staged_rhs=0)
                if i + 2 < UNROLL:
                    stage(query_rows(pairs[i + 2][1]), 0, i % 2)
                pltpu.matmul_acc_lhs(total_of(i), value_columns(old_kt, 1), load_staged_rhs=1)
            for i, _, _, b_m in before:
                settle_sums(i, b_m)
        stage_first(kt, m)
        now_open = tuple(old[3 * i + 2] for i in (UNROLL - 2, UNROLL - 1))
        return kt, m, tuple(v for pair in pairs for v in pair), now_open

    trash = jnp.int32(row_blocks)
    nothing = (jnp.int32(0), jnp.int32(0), trash) * UNROLL
    steps = (total + UNROLL - 1) // UNROLL + 1
    for spare in accs:
        probs[0, : spare.shape[0]] = pltpu.matmul_pop(spare).astype(jnp.bfloat16)
    first = (jnp.int32(0), lows[0])
    stage_first(*first)
    kt, m, _, open_sums = lax.fori_loop(0, steps, body, first + (nothing, (trash, trash)))
    for i in (UNROLL - 2, UNROLL - 1):
        settle_sums(i, open_sums[i - UNROLL + 2])
        for part in range(2):
            probs[i, part * unit : (part + 1) * unit] = pltpu.matmul_pop(ring(i, part)).astype(
                jnp.bfloat16
            )
        pltpu.matmul_acc_lhs(ring(i, 0), jnp.zeros((unit, 256), jnp.bfloat16), load_staged_rhs=0)
        probs[i, :unit] = pltpu.matmul_pop(ring(i, 0)).astype(jnp.bfloat16)

    def finish(m, worst):
        totals = acc[m, HEAD_DIM : HEAD_DIM + 1, :]
        out_ref[m] = (acc[m, :HEAD_DIM, :] * (1.0 / totals)).astype(jnp.bfloat16)
        fine = jnp.logical_and(totals > LEAST_TOTAL, totals < MOST_TOTAL)
        return jnp.maximum(worst, jnp.where(fine, 0.0, 1.0))

    worst = jnp.zeros((1, BLOCK_ROWS), jnp.float32)
    worst = lax.fori_loop(0, row_blocks // 4, four(finish), worst)
    flag[0] = jnp.max(worst)

    @pl.when(flag[0] > 0.0)
    def _():
        def redo(m, carry):
            def masked_scores(kt):
                stage(exact_query_rows(m), 0, 0)
                pltpu.matmul_acc_lhs(score_accs[0][0], key_rows(kt, 0), load_staged_rhs=0)
                pltpu.matmul_acc_lhs(score_accs[0][1], key_rows(kt, 1))
                parts = []
                for part in range(2):
                    scores = pltpu.matmul_pop(score_accs[0][part]) * SCALE
                    met = jnp.clip(last_keys(m) - (kt * KEY_TILE + part * unit), 0, unit)
                    parts.append((scores, iota((unit, BLOCK_ROWS), 0) < met))
                return parts

            def fold_max(kt, peak):
                for scores, allowed in masked_scores(kt):
                    masked = jnp.where(allowed, scores, -3e38)
                    peak = jnp.maximum(peak, jnp.max(masked, axis=0, keepdims=True))
                return peak

            peak = lax.fori_loop(
                0, key_tiles, fold_max, jnp.full((1, BLOCK_ROWS), -3e38, jnp.float32)
            )
            acc[m] = jnp.zeros(acc.shape[1:], jnp.float32)

            def fold_sum(kt, inner):
                for part, (scores, allowed) in enumerate(masked_scores(kt)):
                    p = jnp.where(allowed, jnp.exp(jnp.where(allowed, scores - peak, 0.0)), 0.0)
                    stage(p.astype(jnp.bfloat16), 0, 0)
                    pltpu.matmul_acc_lhs(
                        sum_accs[0][0], value_columns(kt, part), load_staged_rhs=0
                    )
                acc[m] = acc[m] + pltpu.matmul_pop(sum_accs[0][0])
                return inner

            lax.fori_loop(0, key_tiles, fold_sum, 0)
            totals = acc[m, HEAD_DIM : HEAD_DIM + 1, :]
            out_ref[m] = (acc[m, :HEAD_DIM, :] * (1.0 / totals)).astype(jnp.bfloat16)
            return carry

        lax.fori_loop(0, row_blocks, redo, 0)


def attend_call(group, starts, counts, arrived, blocks):
    row_blocks = arrived.shape[0]
    patches = row_blocks * 128
    key_tiles = patches // KEY_TILE
    return pl.pallas_call(
        functools.partial(attend_kernel, blocks),
        out_shape=jax.ShapeDtypeStruct((row_blocks, HEAD_DIM, BLOCK_ROWS), jnp.bfloat16),
        in_specs=[smem(), smem(), vmem(), vmem()],
        out_specs=vmem(),
        scratch_shapes=[
            pltpu.VMEM((patches, 128), jnp.bfloat16),
            pltpu.VMEM((key_tiles, HEAD_DIM + SUM_ROWS, KEY_TILE), jnp.bfloat16),
            pltpu.VMEM((KEY_TILE // 2, 128), jnp.bfloat16),
            pltpu.VMEM((row_blocks + 1, HEAD_DIM + SUM_ROWS, BLOCK_ROWS), jnp.float32),
            pltpu.VMEM((UNROLL, KEY_TILE, BLOCK_ROWS), jnp.bfloat16),
            pltpu.VMEM((row_blocks, 2 * HEAD_DIM, BLOCK_ROWS), jnp.bfloat16),
            pltpu.SMEM((key_tiles + 2 * UNROLL + 2,), jnp.int32),
            pltpu.SMEM((1,), jnp.float32),
        ],
        compiler_params=pltpu.CompilerParams(vmem_limit_bytes=50 * MIB),
        cost_estimate=pl.CostEstimate(
            flops=2 * patches * row_blocks * BLOCK_ROWS * 2 * HEAD_DIM,
            bytes_accessed=2 * 3 * arrived.size // 2,
            transcendentals=patches * row_blocks * BLOCK_ROWS // 2,
        ),
        name="attend",
    )(group, starts, counts, arrived)


def out_kernel(h_ref, w_ref, x_ref, gain_ref, out_ref, rows_in, staged, ins, outs):
    copies = h_ref.shape[0]
    width = w_ref.shape[0]
    load = pltpu.make_async_copy(x_ref, rows_in, ins.at[0])
    load.start()
    sent = []
    for r in range(copies):
        cut = slice(r * BLOCK_ROWS, (r + 1) * BLOCK_ROWS)
        head_out = h_ref[r].reshape(width, BLOCK_ROWS).T
        product = jnp.dot(head_out, w_ref[...], preferred_element_type=jnp.float32)
        if r == 0:
            load.wait()
        residual = rows_in[cut, :].astype(jnp.float32) + product
        staged[cut, :] = norm_rows(residual, gain_ref[...]).astype(jnp.bfloat16)
        where = pl.ds(r * BLOCK_ROWS, BLOCK_ROWS)
        send = pltpu.make_async_copy(staged.at[where], out_ref.at[where], outs.at[r])
        send.start()
        sent.append(send)
    for send in sent:
        send.wait()


def out_call(head_out, w_out, x, gain):
    rows, width = x.shape
    return pl.pallas_call(
        out_kernel,
        out_shape=jax.ShapeDtypeStruct(x.shape, jnp.bfloat16),
        in_specs=[vmem(), vmem(), hbm(), vmem()],
        out_specs=hbm(),
        input_output_aliases={2: 0},
        scratch_shapes=[
            pltpu.VMEM(x.shape, jnp.bfloat16),
            pltpu.VMEM(x.shape, jnp.bfloat16),
            pltpu.SemaphoreType.DMA((1,)),
            pltpu.SemaphoreType.DMA((rows // BLOCK_ROWS,)),
        ],
        compiler_params=pltpu.CompilerParams(vmem_limit_bytes=50 * MIB),
        cost_estimate=pl.CostEstimate(
            flops=2 * rows * width * width, bytes_accessed=2 * (3 * rows * width + width * width),
            transcendentals=rows,
        ),
        name="outputs",
    )(head_out, w_out, x, gain.reshape(1, -1))


def per_device(
    byte_states, patch_latents, patch_lengths, w_down, kv_gain, w_query, w_key, w_value, w_out,
    out_gain,
):
    seqs, mps = lax.axis_size("seq"), lax.axis_size("mp")
    copies = mps // HEADS
    x = byte_states[0]
    patches_here, features = patch_latents.shape[1:]
    part = patches_here // mps

    sent = patch_latents.reshape(seqs * mps, part, features)
    latents = lax.all_to_all(sent, ("seq", "mp"), 0, 0, tiled=True)
    latents = latents.reshape(seqs, mps, part, features)
    lengths = patch_lengths[0].reshape(-1, 128)
    buf, starts, counts, kept = query_call(x, w_query, lengths, mps * x.shape[0])

    buf = kv_call(latents, w_down, kv_gain, w_key, w_value, buf)
    arrived = lax.all_to_all(buf, "mp", 0, 0, tiled=True)

    group = jnp.stack([lax.axis_index("mp") // HEADS, jnp.int32(copies)])
    head_out = attend_call(group, starts, counts, arrived, seqs)
    head_out = lax.all_to_all(head_out, "mp", 0, 0, tiled=True)
    decoded = out_call(
        head_out.reshape(copies, HEADS, HEAD_DIM, BLOCK_ROWS), w_out, kept, out_gain
    )
    return decoded[None]


def solution(mesh):
    return jax.shard_map(
        per_device,
        mesh=mesh,
        in_specs=(
            P("seq", "mp", None),
            P(None, "seq", "mp"),
            P("seq", None),
            P(),
            P(),
            P(),
            P(),
            P(),
            P(),
            P(),
        ),
        out_specs=P("seq", "mp", None),
        check_vma=False,
    )
```

```python
import functools
import math

import jax
import jax.numpy as jnp
from jax import lax
from jax.experimental import pallas as pl
from jax.experimental.pallas import tpu as pltpu
from jax.sharding import PartitionSpec as P

HEADS = 16
HEAD_DIM = 64
BLOCK_ROWS = 256
KEY_TILE = 256
UNROLL = 12
SUM_ROWS = 16
TO_LOG2 = math.log2(math.e) / math.sqrt(HEAD_DIM)
SCALE = 1.0 / math.sqrt(HEAD_DIM)
LEAST_TOTAL = 2.0**-90
MOST_TOTAL = 2.0**110
MIB = 1024 * 1024


def vmem():
    return pl.BlockSpec(memory_space=pltpu.VMEM)


def smem():
    return pl.BlockSpec(memory_space=pltpu.SMEM)


def hbm():
    return pl.BlockSpec(memory_space=pltpu.HBM)


def ones_where(mask):
    return mask.astype(jnp.float32).astype(jnp.bfloat16)


def iota(shape, dim):
    return lax.broadcasted_iota(jnp.int32, shape, dim)


def exact_dot(a, b):
    return jnp.dot(a, b, preferred_element_type=jnp.float32)


def patch_tables(lengths, starts_ref, counts_ref):
    lines, lanes = lengths.shape
    values = lengths.astype(jnp.float32).astype(jnp.bfloat16)
    square = (lanes, lanes)
    within = exact_dot(values, ones_where(iota(square, 0) < iota(square, 1)))
    small = (lines, lines)
    above = exact_dot(ones_where(iota(small, 1) < iota(small, 0)), values)
    starts = (within + jnp.sum(above, axis=1, keepdims=True)).astype(jnp.int32)
    starts_ref[...] = starts
    spots = counts_ref.shape[0]
    tops, lows = [], []
    for line in range(lines):
        row = starts[line : line + 1, :]
        tops.append(ones_where(iota((spots, lanes), 0) == lax.shift_right_logical(row, 7)))
        lows.append(ones_where(iota((128, lanes), 0) == jnp.bitwise_and(row, 127)))
    present = lax.dot_general(
        jnp.concatenate(tops, axis=1),
        jnp.concatenate(lows, axis=1),
        (((1,), (1,)), ((), ())),
        preferred_element_type=jnp.float32,
    ).astype(jnp.bfloat16)
    along = exact_dot(present, ones_where(iota((128, 128), 0) <= iota((128, 128), 1)))
    before = exact_dot(ones_where(iota((spots, spots), 1) < iota((spots, spots), 0)), present)
    counts_ref[...] = (along + jnp.sum(before, axis=1, keepdims=True)).astype(jnp.int32)


def query_kernel(
    x_ref, w_ref, len_ref, buf_ref, starts_ref, counts_ref, kept_ref, staged, sems, keep_sem
):
    rows, width = x_ref.shape
    step = 256
    heads_step = step // HEAD_DIM
    copies = rows // BLOCK_ROWS
    half = BLOCK_ROWS // 128
    keep = pltpu.make_async_copy(x_ref, kept_ref, keep_sem.at[0])
    keep.start()
    sent = [keep]
    for n in range(width // step):
        q = jnp.dot(
            x_ref[...], w_ref[:, n * step : (n + 1) * step], preferred_element_type=jnp.float32
        ).astype(jnp.bfloat16)
        qt = q.T
        for r in range(copies):
            for h in range(heads_step):
                for b in range(half):
                    at = r * BLOCK_ROWS + b * 128
                    staged[r, n * heads_step + h, b * HEAD_DIM : (b + 1) * HEAD_DIM, :] = qt[
                        h * HEAD_DIM : (h + 1) * HEAD_DIM, at : at + 128
                    ]
            cut = pl.ds(n * heads_step, heads_step)
            send = pltpu.make_async_copy(
                staged.at[r, cut],
                buf_ref.at[pl.ds(r * HEADS + n * heads_step, heads_step), pl.ds(128, 128)],
                sems.at[n * copies + r],
            )
            send.start()
            sent.append(send)
    patch_tables(len_ref[...], starts_ref, counts_ref)
    for send in sent:
        send.wait()


def query_call(x, w_query, lengths, seq_len):
    rows, width = x.shape
    copies = rows // BLOCK_ROWS
    return pl.pallas_call(
        query_kernel,
        out_shape=(
            jax.ShapeDtypeStruct((copies * HEADS, 256, 128), jnp.bfloat16),
            jax.ShapeDtypeStruct(lengths.shape, jnp.int32),
            jax.ShapeDtypeStruct((seq_len // 128, 128), jnp.int32),
            jax.ShapeDtypeStruct(x.shape, x.dtype),
        ),
        in_specs=[vmem(), vmem(), vmem()],
        out_specs=(hbm(), vmem(), vmem(), hbm()),
        scratch_shapes=[
            pltpu.VMEM((copies, HEADS, 128, 128), jnp.bfloat16),
            pltpu.SemaphoreType.DMA((copies * width // 256,)),
            pltpu.SemaphoreType.DMA((1,)),
        ],
        compiler_params=pltpu.CompilerParams(vmem_limit_bytes=16 * MIB),
        cost_estimate=pl.CostEstimate(
            flops=2 * rows * width * width, bytes_accessed=2 * (2 * rows * width + width * width),
            transcendentals=0,
        ),
        name="queries",
    )(x, w_query, lengths)


def norm_rows(values, gain):
    mean_square = jnp.mean(values * values, axis=-1, keepdims=True)
    return values * lax.rsqrt(mean_square + 1e-05) * gain.astype(jnp.float32)


WD_PARTS = 8
AHEAD = 5


def kv_kernel(
    x_ref, wd_ref, gain_ref, wk, wv_ref, old_ref, buf_ref, wd, wv, acc, staged, sems, outs
):
    blocks, groups, part, lanes = x_ref.shape
    rows = blocks * part
    depth = wd_ref.shape[0] // WD_PARTS
    per_part = groups // WD_PARTS
    loads = [
        pltpu.make_async_copy(
            wd_ref.at[pl.ds(i * depth, depth)], wd.at[pl.ds(i * depth, depth)], sems.at[i]
        )
        for i in range(WD_PARTS)
    ]
    loads.append(pltpu.make_async_copy(wv_ref, wv, sems.at[WD_PARTS]))
    for load in loads[:AHEAD]:
        load.start()
    for i in range(WD_PARTS):
        if i + AHEAD < len(loads):
            loads[i + AHEAD].start()
        lhs = jnp.concatenate(
            [x_ref[:, i * per_part + g].reshape(rows, lanes) for g in range(per_part)], axis=1
        )
        loads[i].wait()
        product = jnp.dot(
            lhs, wd[i * depth : (i + 1) * depth, :], preferred_element_type=jnp.float32
        )
        acc[...] = product if i == 0 else acc[...] + product
    for load in loads[WD_PARTS + AHEAD :]:
        load.start()
    normed = norm_rows(acc[...], gain_ref[...]).astype(jnp.bfloat16)
    copies = buf_ref.shape[0] // HEADS
    step = 256
    heads_step = step // HEAD_DIM
    acc[...] = jnp.dot(normed, wk[...], preferred_element_type=jnp.float32)
    loads[WD_PARTS].wait()
    sent = []
    for n in range(wv.shape[1] // step):
        cut = slice(n * step, (n + 1) * step)
        keys = acc[:, cut]
        values = jnp.dot(normed, wv[:, cut], preferred_element_type=jnp.float32)
        for h in range(heads_step):
            own = slice(h * HEAD_DIM, (h + 1) * HEAD_DIM)
            staged[n * heads_step + h] = jnp.concatenate(
                [keys[:, own], values[:, own]], axis=1
            ).astype(jnp.bfloat16)
        for r in range(copies):
            send = pltpu.make_async_copy(
                staged.at[pl.ds(n * heads_step, heads_step)],
                buf_ref.at[pl.ds(r * HEADS + n * heads_step, heads_step), pl.ds(0, 128)],
                outs.at[n * copies + r],
            )
            send.start()
            sent.append(send)
    for send in sent:
        send.wait()


def kv_call(x, w_down, gain, w_key, w_value, buf):
    blocks, groups, part, lanes = x.shape
    rows = blocks * part
    width = w_down.shape[1]
    return pl.pallas_call(
        kv_kernel,
        out_shape=jax.ShapeDtypeStruct(buf.shape, buf.dtype),
        in_specs=[vmem(), hbm(), vmem(), vmem(), hbm(), hbm()],
        out_specs=hbm(),
        input_output_aliases={5: 0},
        scratch_shapes=[
            pltpu.VMEM(w_down.shape, jnp.bfloat16),
            pltpu.VMEM(w_value.shape, jnp.bfloat16),
            pltpu.VMEM((rows, width), jnp.float32),
            pltpu.VMEM((HEADS, rows, 2 * HEAD_DIM), jnp.bfloat16),
            pltpu.SemaphoreType.DMA((WD_PARTS + 1,)),
            pltpu.SemaphoreType.DMA((buf.shape[0] // HEADS * width // 256,)),
        ],
        compiler_params=pltpu.CompilerParams(vmem_limit_bytes=47 * MIB),
        cost_estimate=pl.CostEstimate(
            flops=2 * rows * width * (groups * lanes + 2 * width),
            bytes_accessed=2 * (rows * groups * lanes + groups * lanes * width + 2 * width * width),
            transcendentals=0,
        ),
        name="keys_values",
    )(x, w_down, gain.reshape(1, -1), w_key, w_value, buf)


def stage(rhs, register, mxu):
    pltpu.matmul_push_rhs(rhs, staging_register=register, mxu_index=mxu)


def attend_kernel(blocks, *refs):
    unit = KEY_TILE
    kinds = []
    for mxu in range(2):
        kinds += [pltpu.ACC(mxu)((unit, BLOCK_ROWS), jnp.float32)] * 3
        kinds += [pltpu.ACC(mxu)((HEAD_DIM + SUM_ROWS, BLOCK_ROWS), jnp.float32)] * 3
    pl.run_scoped(functools.partial(attend_body, blocks, refs), *kinds)


def attend_body(blocks, refs, *accs):
    group_ref, starts_ref, counts_ref, in_ref, out_ref = refs[:5]
    kvs, vt, order, acc, probs, split, lows, flag = refs[5:]
    score_accs, sum_accs = (accs[0:3], accs[6:9]), (accs[3:6], accs[9:12])
    unit = KEY_TILE
    row_blocks = in_ref.shape[0]
    senders = row_blocks
    part = 128 // blocks
    patches = kvs.shape[0]
    key_tiles = patches // KEY_TILE
    stride = BLOCK_ROWS * group_ref[1]
    group = group_ref[0]

    def ceil_blocks(rows):
        return jnp.minimum((jnp.maximum(rows, 0) + stride - 1) // stride, row_blocks)

    total = jnp.int32(0)
    for kt in range(lows.shape[0]):
        if kt < key_tiles:
            start = starts_ref[kt * KEY_TILE // 128, 0]
            low = ceil_blocks(start - group * BLOCK_ROWS - (BLOCK_ROWS - 1))
            total = total + row_blocks - low
        else:
            low = jnp.int32(row_blocks)
        lows[kt] = low

    for b in range(blocks):
        for s in range(senders):
            at = (b * senders + s) * part
            kvs[at : at + part, :] = in_ref[s, b * part : (b + 1) * part, :]
    sum_row = ones_where(iota((SUM_ROWS, KEY_TILE), 0) == 0)
    for t in range(key_tiles):
        turned = kvs[t * KEY_TILE : (t + 1) * KEY_TILE, :].T
        vt[t, :HEAD_DIM, :] = turned[HEAD_DIM:, :]
        vt[t, HEAD_DIM:, :] = sum_row
    order[...] = iota(order.shape, 0).astype(jnp.float32).astype(jnp.bfloat16)

    lanes = BLOCK_ROWS // 128

    def prepare(m, carry):
        halves = [
            in_ref[m, 128 + b * HEAD_DIM : 128 + (b + 1) * HEAD_DIM, :] for b in range(lanes)
        ]
        scaled = jnp.concatenate(halves, axis=1).astype(jnp.float32) * TO_LOG2
        high = scaled.astype(jnp.bfloat16)
        split[m, :HEAD_DIM, :] = high
        split[m, HEAD_DIM:, :] = (scaled - high.astype(jnp.float32)).astype(jnp.bfloat16)
        acc[m] = jnp.zeros(acc.shape[1:], jnp.float32)
        return carry

    def four(step):
        def steps(i, carry):
            for k in range(4):
                carry = step(4 * i + k, carry)
            return carry

        return steps

    lax.fori_loop(0, row_blocks // 4, four(prepare), 0)
    acc[row_blocks] = jnp.zeros(acc.shape[1:], jnp.float32)

    def query_rows(m):
        gap = jnp.zeros((HEAD_DIM, BLOCK_ROWS), jnp.bfloat16)
        return jnp.concatenate([split[m, :HEAD_DIM, :], gap, split[m, HEAD_DIM:, :], gap], axis=0)

    def exact_query_rows(m):
        halves = [
            in_ref[m, 128 + b * HEAD_DIM : 128 + (b + 1) * HEAD_DIM, :] for b in range(lanes)
        ]
        zeros = jnp.zeros((256 - HEAD_DIM, BLOCK_ROWS), jnp.bfloat16)
        return jnp.concatenate([jnp.concatenate(halves, axis=1), zeros], axis=0)

    def last_keys(m):
        line = (m * stride + group * BLOCK_ROWS) // 128
        met = [counts_ref[pl.ds(line + b, 1), :] for b in range(lanes)]
        return jnp.concatenate(met, axis=1)

    def allowed_keys(m, kt):
        met = jnp.clip(last_keys(m) - kt * KEY_TILE, 0, unit)
        met = met.astype(jnp.float32).astype(jnp.bfloat16)
        return jnp.concatenate([order[...]] * lanes, axis=1) < met

    def key_rows(kt):
        at = pl.multiple_of(kt * KEY_TILE, unit)
        return jnp.concatenate([kvs[pl.ds(at, unit), :]] * 2, axis=1)

    def inside(kt, m):
        return jnp.minimum(kt, key_tiles - 1), jnp.minimum(m, row_blocks - 1)

    def advance(kt, m):
        wrap = m + 1 >= row_blocks
        kt = kt + wrap.astype(jnp.int32)
        return kt, jnp.where(wrap, lows[kt], m + 1)

    def ring(i):
        return score_accs[i % 2][(i // 2) % 3]

    def total_of(i):
        return sum_accs[i % 2][(i // 2) % 3]

    def settle_scores(i, kt, m):
        p = jnp.exp2(pltpu.matmul_pop(ring(i))).astype(jnp.bfloat16)
        probs[i] = jnp.where(allowed_keys(m, kt), p, jnp.zeros_like(p))

    def settle_sums(i, m):
        acc[m] = acc[m] + pltpu.matmul_pop(total_of(i))

    def stage_first(kt, m):
        for mxu in range(2):
            stage(query_rows(inside(kt, m)[1]), 0, mxu)
            kt, m = advance(kt, m)

    left = range(UNROLL - 4, UNROLL)

    def body(_, carry):
        kt, m, old, open_sums = carry
        pairs = []
        for i in range(UNROLL):
            pairs.append(inside(kt, m) + (m,))
            kt, m = advance(kt, m)
        for j in range(0, UNROLL, 2):
            now = (j, j + 1)
            if j < 4:
                before = [
                    (i, old[3 * i], old[3 * i + 1], open_sums[i - UNROLL + 4])
                    for i in (UNROLL - 4 + j, UNROLL - 3 + j)
                ]
            else:
                before = [(i, pairs[i][0], pairs[i][1], old[3 * i + 2]) for i in (j - 4, j - 3)]
            for i in now:
                pltpu.matmul_acc_lhs(ring(i), key_rows(pairs[i][0]), load_staged_rhs=0)
                stage(probs[i], 1, i % 2)
                if i + 2 < UNROLL:
                    stage(query_rows(pairs[i + 2][1]), 0, i % 2)
            for i, b_kt, b_m, _ in before:
                settle_scores(i, b_kt, b_m)
            for i in now:
                pltpu.matmul_acc_lhs(total_of(i), vt[old[3 * i]], load_staged_rhs=1)
            for i, _, _, b_m in before:
                settle_sums(i, b_m)
        stage_first(kt, m)
        now_open = tuple(old[3 * i + 2] for i in left)
        return kt, m, tuple(v for pair in pairs for v in pair), now_open

    trash = jnp.int32(row_blocks)
    nothing = (jnp.int32(0), jnp.int32(0), trash) * UNROLL
    steps = (total + UNROLL - 1) // UNROLL + 1
    for spare in accs:
        probs[0, : spare.shape[0]] = pltpu.matmul_pop(spare).astype(jnp.bfloat16)
    first = (jnp.int32(0), lows[0])
    stage_first(*first)
    kt, m, _, open_sums = lax.fori_loop(0, steps, body, first + (nothing, (trash,) * 4))
    for i in left:
        settle_sums(i, open_sums[i - UNROLL + 4])
        probs[i] = pltpu.matmul_pop(ring(i)).astype(jnp.bfloat16)
    for i in (0, 1):
        pltpu.matmul_acc_lhs(ring(i), jnp.zeros((unit, 256), jnp.bfloat16), load_staged_rhs=0)
        probs[i] = pltpu.matmul_pop(ring(i)).astype(jnp.bfloat16)

    def finish(m, worst):
        totals = acc[m, HEAD_DIM : HEAD_DIM + 1, :]
        out_ref[m] = (acc[m, :HEAD_DIM, :] * (1.0 / totals)).astype(jnp.bfloat16)
        fine = jnp.logical_and(totals > LEAST_TOTAL, totals < MOST_TOTAL)
        return jnp.maximum(worst, jnp.where(fine, 0.0, 1.0))

    worst = jnp.zeros((1, BLOCK_ROWS), jnp.float32)
    worst = lax.fori_loop(0, row_blocks // 4, four(finish), worst)
    flag[0] = jnp.max(worst)

    @pl.when(flag[0] > 0.0)
    def _():
        def redo(m, carry):
            def masked_scores(kt):
                stage(exact_query_rows(m), 0, 0)
                pltpu.matmul_acc_lhs(score_accs[0][0], key_rows(kt), load_staged_rhs=0)
                scores = pltpu.matmul_pop(score_accs[0][0]) * SCALE
                met = jnp.clip(last_keys(m) - kt * KEY_TILE, 0, unit)
                return scores, iota((unit, BLOCK_ROWS), 0) < met

            def fold_max(kt, peak):
                scores, allowed = masked_scores(kt)
                masked = jnp.where(allowed, scores, -3e38)
                return jnp.maximum(peak, jnp.max(masked, axis=0, keepdims=True))

            peak = lax.fori_loop(
                0, key_tiles, fold_max, jnp.full((1, BLOCK_ROWS), -3e38, jnp.float32)
            )
            acc[m] = jnp.zeros(acc.shape[1:], jnp.float32)

            def fold_sum(kt, inner):
                scores, allowed = masked_scores(kt)
                p = jnp.where(allowed, jnp.exp(jnp.where(allowed, scores - peak, 0.0)), 0.0)
                stage(p.astype(jnp.bfloat16), 0, 0)
                pltpu.matmul_acc_lhs(sum_accs[0][0], vt[kt], load_staged_rhs=0)
                acc[m] = acc[m] + pltpu.matmul_pop(sum_accs[0][0])
                return inner

            lax.fori_loop(0, key_tiles, fold_sum, 0)
            totals = acc[m, HEAD_DIM : HEAD_DIM + 1, :]
            out_ref[m] = (acc[m, :HEAD_DIM, :] * (1.0 / totals)).astype(jnp.bfloat16)
            return carry

        lax.fori_loop(0, row_blocks, redo, 0)


def attend_call(group, starts, counts, arrived, blocks):
    row_blocks = arrived.shape[0]
    patches = row_blocks * 128
    key_tiles = patches // KEY_TILE
    return pl.pallas_call(
        functools.partial(attend_kernel, blocks),
        out_shape=jax.ShapeDtypeStruct((row_blocks, HEAD_DIM, BLOCK_ROWS), jnp.bfloat16),
        in_specs=[smem(), smem(), vmem(), vmem()],
        out_specs=vmem(),
        scratch_shapes=[
            pltpu.VMEM((patches, 128), jnp.bfloat16),
            pltpu.VMEM((key_tiles, HEAD_DIM + SUM_ROWS, KEY_TILE), jnp.bfloat16),
            pltpu.VMEM((KEY_TILE, 128), jnp.bfloat16),
            pltpu.VMEM((row_blocks + 1, HEAD_DIM + SUM_ROWS, BLOCK_ROWS), jnp.float32),
            pltpu.VMEM((UNROLL, KEY_TILE, BLOCK_ROWS), jnp.bfloat16),
            pltpu.VMEM((row_blocks, 2 * HEAD_DIM, BLOCK_ROWS), jnp.bfloat16),
            pltpu.SMEM((key_tiles + 2 * UNROLL + 2,), jnp.int32),
            pltpu.SMEM((1,), jnp.float32),
        ],
        compiler_params=pltpu.CompilerParams(vmem_limit_bytes=50 * MIB),
        cost_estimate=pl.CostEstimate(
            flops=2 * patches * row_blocks * BLOCK_ROWS * 2 * HEAD_DIM,
            bytes_accessed=2 * 3 * arrived.size // 2,
            transcendentals=patches * row_blocks * BLOCK_ROWS // 2,
        ),
        name="attend",
    )(group, starts, counts, arrived)


def out_kernel(h_ref, w_ref, x_ref, gain_ref, out_ref, rows_in, staged, ins, outs):
    copies = h_ref.shape[0]
    width = w_ref.shape[0]
    load = pltpu.make_async_copy(x_ref, rows_in, ins.at[0])
    load.start()
    sent = []
    for r in range(copies):
        cut = slice(r * BLOCK_ROWS, (r + 1) * BLOCK_ROWS)
        head_out = h_ref[r].reshape(width, BLOCK_ROWS).T
        product = jnp.dot(head_out, w_ref[...], preferred_element_type=jnp.float32)
        if r == 0:
            load.wait()
        residual = rows_in[cut, :].astype(jnp.float32) + product
        staged[cut, :] = norm_rows(residual, gain_ref[...]).astype(jnp.bfloat16)
        where = pl.ds(r * BLOCK_ROWS, BLOCK_ROWS)
        send = pltpu.make_async_copy(staged.at[where], out_ref.at[where], outs.at[r])
        send.start()
        sent.append(send)
    for send in sent:
        send.wait()


def out_call(head_out, w_out, x, gain):
    rows, width = x.shape
    return pl.pallas_call(
        out_kernel,
        out_shape=jax.ShapeDtypeStruct(x.shape, jnp.bfloat16),
        in_specs=[vmem(), vmem(), hbm(), vmem()],
        out_specs=hbm(),
        input_output_aliases={2: 0},
        scratch_shapes=[
            pltpu.VMEM(x.shape, jnp.bfloat16),
            pltpu.VMEM(x.shape, jnp.bfloat16),
            pltpu.SemaphoreType.DMA((1,)),
            pltpu.SemaphoreType.DMA((rows // BLOCK_ROWS,)),
        ],
        compiler_params=pltpu.CompilerParams(vmem_limit_bytes=50 * MIB),
        cost_estimate=pl.CostEstimate(
            flops=2 * rows * width * width, bytes_accessed=2 * (3 * rows * width + width * width),
            transcendentals=rows,
        ),
        name="outputs",
    )(head_out, w_out, x, gain.reshape(1, -1))


def per_device(
    byte_states, patch_latents, patch_lengths, w_down, kv_gain, w_query, w_key, w_value, w_out,
    out_gain,
):
    seqs, mps = lax.axis_size("seq"), lax.axis_size("mp")
    copies = mps // HEADS
    x = byte_states[0]
    patches_here, features = patch_latents.shape[1:]
    part = patches_here // mps

    sent = patch_latents.reshape(seqs * mps, part, features)
    latents = lax.all_to_all(sent, ("seq", "mp"), 0, 0, tiled=True)
    latents = latents.reshape(seqs, mps, part, features)
    lengths = patch_lengths[0].reshape(-1, 128)
    buf, starts, counts, kept = query_call(x, w_query, lengths, mps * x.shape[0])

    buf = kv_call(latents, w_down, kv_gain, w_key, w_value, buf)
    arrived = lax.all_to_all(buf, "mp", 0, 0, tiled=True)

    group = jnp.stack([lax.axis_index("mp") // HEADS, jnp.int32(copies)])
    head_out = attend_call(group, starts, counts, arrived, seqs)
    head_out = lax.all_to_all(head_out, "mp", 0, 0, tiled=True)
    decoded = out_call(
        head_out.reshape(copies, HEADS, HEAD_DIM, BLOCK_ROWS), w_out, kept, out_gain
    )
    return decoded[None]


def solution(mesh):
    return jax.shard_map(
        per_device,
        mesh=mesh,
        in_specs=(
            P("seq", "mp", None),
            P(None, "seq", "mp"),
            P("seq", None),
            P(),
            P(),
            P(),
            P(),
            P(),
            P(),
            P(),
        ),
        out_specs=P("seq", "mp", None),
        check_vma=False,
    )
```

```python
import functools
import math

import jax
import jax.numpy as jnp
from jax import lax
from jax.experimental import pallas as pl
from jax.experimental.pallas import tpu as pltpu
from jax.sharding import PartitionSpec as P

HEADS = 16
HEAD_DIM = 64
BLOCK_ROWS = 256
KEY_TILE = 256
UNROLL = 12
SUM_ROWS = 16
TO_LOG2 = math.log2(math.e) / math.sqrt(HEAD_DIM)
SCALE = 1.0 / math.sqrt(HEAD_DIM)
LEAST_TOTAL = 2.0**-90
MOST_TOTAL = 2.0**110
MIB = 1024 * 1024


def vmem():
    return pl.BlockSpec(memory_space=pltpu.VMEM)


def smem():
    return pl.BlockSpec(memory_space=pltpu.SMEM)


def hbm():
    return pl.BlockSpec(memory_space=pltpu.HBM)


def ones_where(mask):
    return mask.astype(jnp.float32).astype(jnp.bfloat16)


def iota(shape, dim):
    return lax.broadcasted_iota(jnp.int32, shape, dim)


def exact_dot(a, b):
    return jnp.dot(a, b, preferred_element_type=jnp.float32)


def patch_tables(lengths, starts_ref, counts_ref):
    lines, lanes = lengths.shape
    values = lengths.astype(jnp.float32).astype(jnp.bfloat16)
    square = (lanes, lanes)
    within = exact_dot(values, ones_where(iota(square, 0) < iota(square, 1)))
    small = (lines, lines)
    above = exact_dot(ones_where(iota(small, 1) < iota(small, 0)), values)
    starts = (within + jnp.sum(above, axis=1, keepdims=True)).astype(jnp.int32)
    starts_ref[...] = starts
    spots = counts_ref.shape[0]
    tops, lows = [], []
    for line in range(lines):
        row = starts[line : line + 1, :]
        tops.append(ones_where(iota((spots, lanes), 0) == lax.shift_right_logical(row, 7)))
        lows.append(ones_where(iota((128, lanes), 0) == jnp.bitwise_and(row, 127)))
    present = lax.dot_general(
        jnp.concatenate(tops, axis=1),
        jnp.concatenate(lows, axis=1),
        (((1,), (1,)), ((), ())),
        preferred_element_type=jnp.float32,
    ).astype(jnp.bfloat16)
    along = exact_dot(present, ones_where(iota((128, 128), 0) <= iota((128, 128), 1)))
    before = exact_dot(ones_where(iota((spots, spots), 1) < iota((spots, spots), 0)), present)
    counts_ref[...] = (along + jnp.sum(before, axis=1, keepdims=True)).astype(jnp.int32)


def query_kernel(
    x_ref, w_ref, len_ref, buf_ref, starts_ref, counts_ref, kept_ref, staged, sems, keep_sem
):
    rows, width = x_ref.shape
    step = 256
    heads_step = step // HEAD_DIM
    copies = rows // BLOCK_ROWS
    half = BLOCK_ROWS // 128
    keep = pltpu.make_async_copy(x_ref, kept_ref, keep_sem.at[0])
    keep.start()
    sent = [keep]
    for n in range(width // step):
        q = jnp.dot(
            x_ref[...], w_ref[:, n * step : (n + 1) * step], preferred_element_type=jnp.float32
        ).astype(jnp.bfloat16)
        qt = q.T
        for r in range(copies):
            for h in range(heads_step):
                for b in range(half):
                    at = r * BLOCK_ROWS + b * 128
                    staged[r, n * heads_step + h, b * HEAD_DIM : (b + 1) * HEAD_DIM, :] = qt[
                        h * HEAD_DIM : (h + 1) * HEAD_DIM, at : at + 128
                    ]
            cut = pl.ds(n * heads_step, heads_step)
            send = pltpu.make_async_copy(
                staged.at[r, cut],
                buf_ref.at[pl.ds(r * HEADS + n * heads_step, heads_step), pl.ds(128, 128)],
                sems.at[n * copies + r],
            )
            send.start()
            sent.append(send)
    patch_tables(len_ref[...], starts_ref, counts_ref)
    for send in sent:
        send.wait()


def query_call(x, w_query, lengths, seq_len):
    rows, width = x.shape
    copies = rows // BLOCK_ROWS
    return pl.pallas_call(
        query_kernel,
        out_shape=(
            jax.ShapeDtypeStruct((copies * HEADS, 256, 128), jnp.bfloat16),
            jax.ShapeDtypeStruct(lengths.shape, jnp.int32),
            jax.ShapeDtypeStruct((seq_len // 128, 128), jnp.int32),
            jax.ShapeDtypeStruct(x.shape, x.dtype),
        ),
        in_specs=[vmem(), vmem(), vmem()],
        out_specs=(hbm(), vmem(), vmem(), hbm()),
        scratch_shapes=[
            pltpu.VMEM((copies, HEADS, 128, 128), jnp.bfloat16),
            pltpu.SemaphoreType.DMA((copies * width // 256,)),
            pltpu.SemaphoreType.DMA((1,)),
        ],
        compiler_params=pltpu.CompilerParams(vmem_limit_bytes=16 * MIB),
        cost_estimate=pl.CostEstimate(
            flops=2 * rows * width * width, bytes_accessed=2 * (2 * rows * width + width * width),
            transcendentals=0,
        ),
        name="queries",
    )(x, w_query, lengths)


def norm_rows(values, gain):
    mean_square = jnp.mean(values * values, axis=-1, keepdims=True)
    return values * lax.rsqrt(mean_square + 1e-05) * gain.astype(jnp.float32)


WD_PARTS = 8
AHEAD = 7


def kv_kernel(
    x_ref, wd_ref, gain_ref, wk, wv_ref, old_ref, buf_ref, wd, wv, acc, staged, sems, outs
):
    blocks, groups, part, lanes = x_ref.shape
    rows = blocks * part
    depth = wd_ref.shape[0] // WD_PARTS
    per_part = groups // WD_PARTS
    loads = [
        pltpu.make_async_copy(
            wd_ref.at[pl.ds(i * depth, depth)], wd.at[pl.ds(i * depth, depth)], sems.at[i]
        )
        for i in range(WD_PARTS)
    ]
    loads.append(pltpu.make_async_copy(wv_ref, wv, sems.at[WD_PARTS]))
    for load in loads[:AHEAD]:
        load.start()
    for i in range(WD_PARTS):
        if i + AHEAD < len(loads):
            loads[i + AHEAD].start()
        lhs = jnp.concatenate(
            [x_ref[:, i * per_part + g].reshape(rows, lanes) for g in range(per_part)], axis=1
        )
        loads[i].wait()
        product = jnp.dot(
            lhs, wd[i * depth : (i + 1) * depth, :], preferred_element_type=jnp.float32
        )
        acc[...] = product if i == 0 else acc[...] + product
    for load in loads[WD_PARTS + AHEAD :]:
        load.start()
    normed = norm_rows(acc[...], gain_ref[...]).astype(jnp.bfloat16)
    copies = buf_ref.shape[0] // HEADS
    step = 256
    heads_step = step // HEAD_DIM
    acc[...] = jnp.dot(normed, wk[...], preferred_element_type=jnp.float32)
    loads[WD_PARTS].wait()
    sent = []
    for n in range(wv.shape[1] // step):
        cut = slice(n * step, (n + 1) * step)
        keys = acc[:, cut]
        values = jnp.dot(normed, wv[:, cut], preferred_element_type=jnp.float32)
        for h in range(heads_step):
            own = slice(h * HEAD_DIM, (h + 1) * HEAD_DIM)
            staged[n * heads_step + h] = jnp.concatenate(
                [keys[:, own], values[:, own]], axis=1
            ).astype(jnp.bfloat16)
        for r in range(copies):
            send = pltpu.make_async_copy(
                staged.at[pl.ds(n * heads_step, heads_step)],
                buf_ref.at[pl.ds(r * HEADS + n * heads_step, heads_step), pl.ds(0, 128)],
                outs.at[n * copies + r],
            )
            send.start()
            sent.append(send)
    for send in sent:
        send.wait()


def kv_call(x, w_down, gain, w_key, w_value, buf):
    blocks, groups, part, lanes = x.shape
    rows = blocks * part
    width = w_down.shape[1]
    return pl.pallas_call(
        kv_kernel,
        out_shape=jax.ShapeDtypeStruct(buf.shape, buf.dtype),
        in_specs=[vmem(), hbm(), vmem(), vmem(), hbm(), hbm()],
        out_specs=hbm(),
        input_output_aliases={5: 0},
        scratch_shapes=[
            pltpu.VMEM(w_down.shape, jnp.bfloat16),
            pltpu.VMEM(w_value.shape, jnp.bfloat16),
            pltpu.VMEM((rows, width), jnp.float32),
            pltpu.VMEM((HEADS, rows, 2 * HEAD_DIM), jnp.bfloat16),
            pltpu.SemaphoreType.DMA((WD_PARTS + 1,)),
            pltpu.SemaphoreType.DMA((buf.shape[0] // HEADS * width // 256,)),
        ],
        compiler_params=pltpu.CompilerParams(vmem_limit_bytes=47 * MIB),
        cost_estimate=pl.CostEstimate(
            flops=2 * rows * width * (groups * lanes + 2 * width),
            bytes_accessed=2 * (rows * groups * lanes + groups * lanes * width + 2 * width * width),
            transcendentals=0,
        ),
        name="keys_values",
    )(x, w_down, gain.reshape(1, -1), w_key, w_value, buf)


def stage(rhs, register, mxu):
    pltpu.matmul_push_rhs(rhs, staging_register=register, mxu_index=mxu)


def attend_kernel(blocks, *refs):
    unit = KEY_TILE
    kinds = []
    for mxu in range(2):
        kinds += [pltpu.ACC(mxu)((unit, BLOCK_ROWS), jnp.float32)] * 3
        kinds += [pltpu.ACC(mxu)((HEAD_DIM + SUM_ROWS, BLOCK_ROWS), jnp.float32)] * 3
    pl.run_scoped(functools.partial(attend_body, blocks, refs), *kinds)


def attend_body(blocks, refs, *accs):
    group_ref, starts_ref, counts_ref, in_ref, out_ref = refs[:5]
    kvs, vt, order, acc, probs, split, lows, flag = refs[5:]
    score_accs, sum_accs = (accs[0:3], accs[6:9]), (accs[3:6], accs[9:12])
    unit = KEY_TILE
    row_blocks = in_ref.shape[0]
    senders = row_blocks
    part = 128 // blocks
    patches = kvs.shape[0]
    key_tiles = patches // KEY_TILE
    stride = BLOCK_ROWS * group_ref[1]
    group = group_ref[0]

    def ceil_blocks(rows):
        return jnp.minimum((jnp.maximum(rows, 0) + stride - 1) // stride, row_blocks)

    total = jnp.int32(0)
    for kt in range(lows.shape[0]):
        if kt < key_tiles:
            start = starts_ref[kt * KEY_TILE // 128, 0]
            low = ceil_blocks(start - group * BLOCK_ROWS - (BLOCK_ROWS - 1))
            total = total + row_blocks - low
        else:
            low = jnp.int32(row_blocks)
        lows[kt] = low

    for b in range(blocks):
        for s in range(senders):
            at = (b * senders + s) * part
            kvs[at : at + part, :] = in_ref[s, b * part : (b + 1) * part, :]
    sum_row = ones_where(iota((SUM_ROWS, KEY_TILE), 0) == 0)
    for t in range(key_tiles):
        turned = kvs[t * KEY_TILE : (t + 1) * KEY_TILE, :].T
        vt[t, :HEAD_DIM, :] = turned[HEAD_DIM:, :]
        vt[t, HEAD_DIM:, :] = sum_row
    order[...] = iota(order.shape, 0).astype(jnp.float32).astype(jnp.bfloat16)

    lanes = BLOCK_ROWS // 128

    def prepare(m, carry):
        halves = [
            in_ref[m, 128 + b * HEAD_DIM : 128 + (b + 1) * HEAD_DIM, :] for b in range(lanes)
        ]
        scaled = jnp.concatenate(halves, axis=1).astype(jnp.float32) * TO_LOG2
        high = scaled.astype(jnp.bfloat16)
        split[m, :HEAD_DIM, :] = high
        split[m, HEAD_DIM:, :] = (scaled - high.astype(jnp.float32)).astype(jnp.bfloat16)
        acc[m] = jnp.zeros(acc.shape[1:], jnp.float32)
        return carry

    def four(step):
        def steps(i, carry):
            for k in range(4):
                carry = step(4 * i + k, carry)
            return carry

        return steps

    lax.fori_loop(0, row_blocks // 4, four(prepare), 0)
    acc[row_blocks] = jnp.zeros(acc.shape[1:], jnp.float32)

    def query_rows(m):
        gap = jnp.zeros((HEAD_DIM, BLOCK_ROWS), jnp.bfloat16)
        return jnp.concatenate([split[m, :HEAD_DIM, :], gap, split[m, HEAD_DIM:, :], gap], axis=0)

    def exact_query_rows(m):
        halves = [
            in_ref[m, 128 + b * HEAD_DIM : 128 + (b + 1) * HEAD_DIM, :] for b in range(lanes)
        ]
        zeros = jnp.zeros((256 - HEAD_DIM, BLOCK_ROWS), jnp.bfloat16)
        return jnp.concatenate([jnp.concatenate(halves, axis=1), zeros], axis=0)

    def last_keys(m):
        line = (m * stride + group * BLOCK_ROWS) // 128
        met = [counts_ref[pl.ds(line + b, 1), :] for b in range(lanes)]
        return jnp.concatenate(met, axis=1)

    def allowed_keys(m, kt):
        met = jnp.clip(last_keys(m) - kt * KEY_TILE, 0, unit)
        met = met.astype(jnp.float32).astype(jnp.bfloat16)
        return jnp.concatenate([order[...]] * lanes, axis=1) < met

    def key_rows(kt):
        at = pl.multiple_of(kt * KEY_TILE, unit)
        return jnp.concatenate([kvs[pl.ds(at, unit), :]] * 2, axis=1)

    def inside(kt, m):
        return jnp.minimum(kt, key_tiles - 1), jnp.minimum(m, row_blocks - 1)

    def advance(kt, m):
        wrap = m + 1 >= row_blocks
        kt = kt + wrap.astype(jnp.int32)
        return kt, jnp.where(wrap, lows[kt], m + 1)

    def ring(i):
        return score_accs[i % 2][(i // 2) % 3]

    def total_of(i):
        return sum_accs[i % 2][(i // 2) % 3]

    def settle_scores(i, kt, m):
        p = jnp.exp2(pltpu.matmul_pop(ring(i))).astype(jnp.bfloat16)
        probs[i] = jnp.where(allowed_keys(m, kt), p, jnp.zeros_like(p))

    def settle_sums(i, m):
        acc[m] = acc[m] + pltpu.matmul_pop(total_of(i))

    def stage_first(kt, m):
        for mxu in range(2):
            stage(query_rows(inside(kt, m)[1]), 0, mxu)
            kt, m = advance(kt, m)

    left = range(UNROLL - 4, UNROLL)

    def body(_, carry):
        kt, m, old, open_sums = carry
        pairs = []
        for i in range(UNROLL):
            pairs.append(inside(kt, m) + (m,))
            kt, m = advance(kt, m)
        for j in range(0, UNROLL, 2):
            now = (j, j + 1)
            if j < 4:
                before = [
                    (i, old[3 * i], old[3 * i + 1], open_sums[i - UNROLL + 4])
                    for i in (UNROLL - 4 + j, UNROLL - 3 + j)
                ]
            else:
                before = [(i, pairs[i][0], pairs[i][1], old[3 * i + 2]) for i in (j - 4, j - 3)]
            for i in now:
                pltpu.matmul_acc_lhs(ring(i), key_rows(pairs[i][0]), load_staged_rhs=0)
                stage(probs[i], 1, i % 2)
                if i + 2 < UNROLL:
                    stage(query_rows(pairs[i + 2][1]), 0, i % 2)
            for i, b_kt, b_m, _ in before:
                settle_scores(i, b_kt, b_m)
            for i in now:
                pltpu.matmul_acc_lhs(total_of(i), vt[old[3 * i]], load_staged_rhs=1)
            for i, _, _, b_m in before:
                settle_sums(i, b_m)
        stage_first(kt, m)
        now_open = tuple(old[3 * i + 2] for i in left)
        return kt, m, tuple(v for pair in pairs for v in pair), now_open

    trash = jnp.int32(row_blocks)
    nothing = (jnp.int32(0), jnp.int32(0), trash) * UNROLL
    steps = (total + UNROLL - 1) // UNROLL + 1
    for spare in accs:
        probs[0, : spare.shape[0]] = pltpu.matmul_pop(spare).astype(jnp.bfloat16)
    first = (jnp.int32(0), lows[0])
    stage_first(*first)
    kt, m, _, open_sums = lax.fori_loop(0, steps, body, first + (nothing, (trash,) * 4))
    for i in left:
        settle_sums(i, open_sums[i - UNROLL + 4])
        probs[i] = pltpu.matmul_pop(ring(i)).astype(jnp.bfloat16)
    for i in (0, 1):
        pltpu.matmul_acc_lhs(ring(i), jnp.zeros((unit, 256), jnp.bfloat16), load_staged_rhs=0)
        probs[i] = pltpu.matmul_pop(ring(i)).astype(jnp.bfloat16)

    def finish(m, worst):
        totals = acc[m, HEAD_DIM : HEAD_DIM + 1, :]
        out_ref[m] = (acc[m, :HEAD_DIM, :] * (1.0 / totals)).astype(jnp.bfloat16)
        fine = jnp.logical_and(totals > LEAST_TOTAL, totals < MOST_TOTAL)
        return jnp.maximum(worst, jnp.where(fine, 0.0, 1.0))

    worst = jnp.zeros((1, BLOCK_ROWS), jnp.float32)
    worst = lax.fori_loop(0, row_blocks // 4, four(finish), worst)
    flag[0] = jnp.max(worst)

    @pl.when(flag[0] > 0.0)
    def _():
        def redo(m, carry):
            def masked_scores(kt):
                stage(exact_query_rows(m), 0, 0)
                pltpu.matmul_acc_lhs(score_accs[0][0], key_rows(kt), load_staged_rhs=0)
                scores = pltpu.matmul_pop(score_accs[0][0]) * SCALE
                met = jnp.clip(last_keys(m) - kt * KEY_TILE, 0, unit)
                return scores, iota((unit, BLOCK_ROWS), 0) < met

            def fold_max(kt, peak):
                scores, allowed = masked_scores(kt)
                masked = jnp.where(allowed, scores, -3e38)
                return jnp.maximum(peak, jnp.max(masked, axis=0, keepdims=True))

            peak = lax.fori_loop(
                0, key_tiles, fold_max, jnp.full((1, BLOCK_ROWS), -3e38, jnp.float32)
            )
            acc[m] = jnp.zeros(acc.shape[1:], jnp.float32)

            def fold_sum(kt, inner):
                scores, allowed = masked_scores(kt)
                p = jnp.where(allowed, jnp.exp(jnp.where(allowed, scores - peak, 0.0)), 0.0)
                stage(p.astype(jnp.bfloat16), 0, 0)
                pltpu.matmul_acc_lhs(sum_accs[0][0], vt[kt], load_staged_rhs=0)
                acc[m] = acc[m] + pltpu.matmul_pop(sum_accs[0][0])
                return inner

            lax.fori_loop(0, key_tiles, fold_sum, 0)
            totals = acc[m, HEAD_DIM : HEAD_DIM + 1, :]
            out_ref[m] = (acc[m, :HEAD_DIM, :] * (1.0 / totals)).astype(jnp.bfloat16)
            return carry

        lax.fori_loop(0, row_blocks, redo, 0)


def attend_call(group, starts, counts, arrived, blocks):
    row_blocks = arrived.shape[0]
    patches = row_blocks * 128
    key_tiles = patches // KEY_TILE
    return pl.pallas_call(
        functools.partial(attend_kernel, blocks),
        out_shape=jax.ShapeDtypeStruct((row_blocks, HEAD_DIM, BLOCK_ROWS), jnp.bfloat16),
        in_specs=[smem(), smem(), vmem(), vmem()],
        out_specs=vmem(),
        scratch_shapes=[
            pltpu.VMEM((patches, 128), jnp.bfloat16),
            pltpu.VMEM((key_tiles, HEAD_DIM + SUM_ROWS, KEY_TILE), jnp.bfloat16),
            pltpu.VMEM((KEY_TILE, 128), jnp.bfloat16),
            pltpu.VMEM((row_blocks + 1, HEAD_DIM + SUM_ROWS, BLOCK_ROWS), jnp.float32),
            pltpu.VMEM((UNROLL, KEY_TILE, BLOCK_ROWS), jnp.bfloat16),
            pltpu.VMEM((row_blocks, 2 * HEAD_DIM, BLOCK_ROWS), jnp.bfloat16),
            pltpu.SMEM((key_tiles + 2 * UNROLL + 2,), jnp.int32),
            pltpu.SMEM((1,), jnp.float32),
        ],
        compiler_params=pltpu.CompilerParams(vmem_limit_bytes=50 * MIB),
        cost_estimate=pl.CostEstimate(
            flops=2 * patches * row_blocks * BLOCK_ROWS * 2 * HEAD_DIM,
            bytes_accessed=2 * 3 * arrived.size // 2,
            transcendentals=patches * row_blocks * BLOCK_ROWS // 2,
        ),
        name="attend",
    )(group, starts, counts, arrived)


def out_kernel(h_ref, w_ref, x_ref, gain_ref, out_ref, rows_in, staged, ins, outs):
    copies = h_ref.shape[0]
    width = w_ref.shape[0]
    load = pltpu.make_async_copy(x_ref, rows_in, ins.at[0])
    load.start()
    sent = []
    for r in range(copies):
        cut = slice(r * BLOCK_ROWS, (r + 1) * BLOCK_ROWS)
        head_out = h_ref[r].reshape(width, BLOCK_ROWS).T
        product = jnp.dot(head_out, w_ref[...], preferred_element_type=jnp.float32)
        if r == 0:
            load.wait()
        residual = rows_in[cut, :].astype(jnp.float32) + product
        staged[cut, :] = norm_rows(residual, gain_ref[...]).astype(jnp.bfloat16)
        where = pl.ds(r * BLOCK_ROWS, BLOCK_ROWS)
        send = pltpu.make_async_copy(staged.at[where], out_ref.at[where], outs.at[r])
        send.start()
        sent.append(send)
    for send in sent:
        send.wait()


def out_call(head_out, w_out, x, gain):
    rows, width = x.shape
    return pl.pallas_call(
        out_kernel,
        out_shape=jax.ShapeDtypeStruct(x.shape, jnp.bfloat16),
        in_specs=[vmem(), vmem(), hbm(), vmem()],
        out_specs=hbm(),
        input_output_aliases={2: 0},
        scratch_shapes=[
            pltpu.VMEM(x.shape, jnp.bfloat16),
            pltpu.VMEM(x.shape, jnp.bfloat16),
            pltpu.SemaphoreType.DMA((1,)),
            pltpu.SemaphoreType.DMA((rows // BLOCK_ROWS,)),
        ],
        compiler_params=pltpu.CompilerParams(vmem_limit_bytes=50 * MIB),
        cost_estimate=pl.CostEstimate(
            flops=2 * rows * width * width, bytes_accessed=2 * (3 * rows * width + width * width),
            transcendentals=rows,
        ),
        name="outputs",
    )(head_out, w_out, x, gain.reshape(1, -1))


def per_device(
    byte_states, patch_latents, patch_lengths, w_down, kv_gain, w_query, w_key, w_value, w_out,
    out_gain,
):
    seqs, mps = lax.axis_size("seq"), lax.axis_size("mp")
    copies = mps // HEADS
    x = byte_states[0]
    patches_here, features = patch_latents.shape[1:]
    part = patches_here // mps

    sent = patch_latents.reshape(seqs * mps, part, features)
    latents = lax.all_to_all(sent, ("seq", "mp"), 0, 0, tiled=True)
    latents = latents.reshape(seqs, mps, part, features)
    lengths = patch_lengths[0].reshape(-1, 128)
    buf, starts, counts, kept = query_call(x, w_query, lengths, mps * x.shape[0])

    buf = kv_call(latents, w_down, kv_gain, w_key, w_value, buf)
    arrived = lax.all_to_all(buf, "mp", 0, 0, tiled=True)

    group = jnp.stack([lax.axis_index("mp") // HEADS, jnp.int32(copies)])
    head_out = attend_call(group, starts, counts, arrived, seqs)
    head_out = lax.all_to_all(head_out, "mp", 0, 0, tiled=True)
    decoded = out_call(
        head_out.reshape(copies, HEADS, HEAD_DIM, BLOCK_ROWS), w_out, kept, out_gain
    )
    return decoded[None]


def solution(mesh):
    return jax.shard_map(
        per_device,
        mesh=mesh,
        in_specs=(
            P("seq", "mp", None),
            P(None, "seq", "mp"),
            P("seq", None),
            P(),
            P(),
            P(),
            P(),
            P(),
            P(),
            P(),
        ),
        out_specs=P("seq", "mp", None),
        check_vma=False,
    )
```
